512 devices in a mesh: prow: 8 (over z), pcol: 64 (over y, x, core).
Axes of the slice: x: 4, y: 8, z: 8, core: 2. Of those that a mesh axis runs over, the one named last changes fastest.
Arguments:
- vectors: float32 [32768, 8192], P('prow', 'pcol'), may hold values from -6 to 6
- reflectors: bfloat16 [4, 256, 32768], P(None, 'pcol', 'prow'), may hold values from -0.03125 to 0.03125
- tau_diag: float32 [4, 256], replicated, may hold values from 0.5 to 1.5
- coupling: float32 [4, 256, 256], replicated, may hold values from -0.375 to 0.375
Outputs:
- result: float32 [32768, 8192], P('prow', 'pcol')
The draws below stay inside these ranges and needn't reach their ends.
All inputs are finite; a program needn't handle non-finite values.
Results may differ from the reference program's by a relative error of at most 0.0003.
Values may be sent and summed in bfloat16 or wider, within the bound.
No kernel may reach another device: no remote copies, remote signals or barrier semaphores. Data moves between devices by JAX's collectives and lax.ppermute only.
A program may use at most 64 MiB of HBM per device.

```python
import jax
import jax.numpy as jnp
from jax import lax

N = 32768
NB = 256
PANELS = 4
M = 8192


def steps_of(own_key, extent, pieces, low, top_value):
    def one(dim, parts):
        heights = jax.random.uniform(jax.random.fold_in(jax.random.fold_in(own_key, 6), dim), (parts,), jnp.float32, low / len(pieces), top_value / len(pieces))
        return jnp.repeat(jnp.exp(heights), extent[dim] // parts).reshape((-1,) + (1,) * (len(extent) - dim - 1))

    loudness = one(*pieces[0])
    for cut in pieces[1:]:
        loudness = loudness * one(*cut)
    return loudness


def scatter_about(rng, extent, spread, reach, shards=(), kind=jnp.bfloat16):
    entries = jax.random.normal(rng, extent, jnp.float32) * spread
    if len(shards) > 0:
        entries = steps_of(rng, extent, shards, -0.22, 0.18) * entries
    return jnp.clip(entries, min=-reach, max=reach).astype(kind)


def setup_inputs(seed: int = 0) -> dict:
    streams_of = jax.random.split(jax.random.key(seed), 5)
    return {
        "vectors": scatter_about(streams_of[0], (N, M), 1.0, 6.0, ((0, 8), (1, 64)), jnp.float32),
        "reflectors": scatter_about(streams_of[1], (PANELS, NB, N), N ** -0.5, 0.03125, ((1, 64), (2, 8))),
        "tau_diag": jnp.clip(jax.random.uniform(streams_of[2], (PANELS, NB), jnp.float32, 0.5, 1.5), 0.5, 1.5),
        "coupling": scatter_about(streams_of[3], (PANELS, NB, NB), NB ** -0.5, 0.375, (), jnp.float32),
    }


def reference(vectors, reflectors, tau_diag, coupling):
    current = vectors
    for position in range(PANELS - 1, -1, -1):
        widened = reflectors[position].astype(jnp.float32)
        tri_factor = jnp.diag(tau_diag[position]) + jnp.triu(coupling[position], 1)
        products = jnp.dot(widened, current, precision=lax.Precision.HIGHEST, preferred_element_type=jnp.float32)
        updates = jnp.dot(tri_factor, products, precision=lax.Precision.HIGHEST, preferred_element_type=jnp.float32)
        current = current - jnp.dot(widened.T, updates, precision=lax.Precision.HIGHEST, preferred_element_type=jnp.float32)
    return current
```

```python
import jax
import jax.numpy as jnp
from jax import lax
from jax.sharding import Mesh
from jax.sharding import PartitionSpec as P

PCOL = ("pcol_0", "pcol_1", "pcol_2")


def exchange(parts, axis):
    return lax.all_to_all(parts, axis, split_axis=0, concat_axis=0, tiled=True)


def copy_for_each(x, axis, devices):
    return exchange(jnp.broadcast_to(x, (devices, *x.shape)), axis)


def from_partner(x):
    return lax.ppermute(x, "pcol_2", [(0, 1), (1, 0)])


def two_terms(x):
    high = lax.reduce_precision(x, exponent_bits=8, mantissa_bits=7)
    return high.astype(jnp.bfloat16), (x - high).astype(jnp.bfloat16)


def products(half, terms):
    both = jnp.dot(half, terms, preferred_element_type=jnp.float32)
    columns = terms.shape[1] // 2
    return both[:, :columns] + both[:, columns:]


def spread(half, image):
    high, low = two_terms(image)
    dims = (((0,), (0,)), ((), ()))
    return lax.dot_general(half, high, dims, preferred_element_type=jnp.float32) + lax.dot_general(
        half, low, dims, preferred_element_type=jnp.float32
    )


def sum_everywhere(x, axis):
    devices = lax.axis_size(axis)
    arrived = exchange(x.reshape(devices, x.shape[0] // devices, x.shape[1]), axis)
    return copy_for_each(arrived.sum(axis=0), axis, devices).reshape(x.shape)


def reordered(tri_factor, outer, core, inner):
    size = tri_factor.shape[0]
    place = lax.broadcasted_iota(jnp.int32, (size, size), 0)
    source = lax.broadcasted_iota(jnp.int32, (size, size), 1)
    part, rest = place // (outer * inner), place % (outer * inner)
    owner = jnp.where(part == 0, core, 1 - core)
    wanted = ((rest // inner) * 2 + owner) * inner + rest % inner
    choose = (wanted == source).astype(jnp.float32)
    turned = jnp.dot(choose, tri_factor, precision=lax.Precision.HIGHEST)
    return lax.dot_general(turned, choose, (((1,), (1,)), ((), ())), precision=lax.Precision.HIGHEST)


def on_device(vectors, reflectors, tau_diag, coupling):
    count, each, rows = reflectors.shape
    high_axis, low_axis, core_axis = PCOL
    wide, deep = lax.axis_size(high_axis), lax.axis_size(low_axis)
    core = lax.axis_index(core_axis)
    last = count - 1

    early = copy_for_each(reflectors[:last], low_axis, deep)
    early = early.transpose(1, 0, 2, 3).reshape(last, deep * each, rows)
    later = lax.all_gather(early, high_axis, axis=0, tiled=False)

    first = copy_for_each(reflectors[last], (high_axis, low_axis), wide * deep)
    first = first.reshape(wide * deep * each, rows)

    current = vectors
    for position in range(last, -1, -1):
        own = first if position == last else later[:, position].reshape(-1, rows)
        other = from_partner(own)
        tri_factor = jnp.diag(tau_diag[position]) + jnp.triu(coupling[position], 1)
        tri_factor = reordered(tri_factor, wide * deep, core, each)
        terms = jnp.concatenate(two_terms(current), axis=1)
        partial_sum = jnp.concatenate([products(own, terms), products(other, terms)], axis=0)
        total = sum_everywhere(partial_sum, "prow")
        image = jnp.dot(tri_factor, total, precision=lax.Precision.HIGHEST)
        split = image.shape[0] // 2
        current = current - spread(own, image[:split]) - spread(other, image[split:])
    return current


def solution(mesh):
    finer = Mesh(
        mesh.devices.reshape(mesh.shape["prow"], 8, 4, 2), ("prow", "pcol_0", "pcol_1", "pcol_2")
    )
    placed = (P("prow", PCOL), P(None, PCOL, "prow"), P(), P())
    return jax.shard_map(
        on_device, mesh=finer, in_specs=placed, out_specs=P("prow", PCOL), check_vma=False
    )
```

```python
import functools

import jax
import jax.numpy as jnp
from jax import lax
from jax.experimental import pallas as pl
from jax.experimental.pallas import tpu as pltpu
from jax.sharding import Mesh
from jax.sharding import PartitionSpec as P

PCOL = ("pcol_0", "pcol_1", "pcol_2")
CHUNK = 512
ROWS_BY_LANES = (((1,), (1,)), ((), ()))


def exchange(parts, axis):
    return lax.all_to_all(parts, axis, split_axis=0, concat_axis=0, tiled=True)


def copy_for_each(x, axis, devices):
    return exchange(jnp.broadcast_to(x, (devices, *x.shape)), axis)


def from_partner(x):
    return lax.ppermute(x, "pcol_2", [(0, 1), (1, 0)])


def two_terms(x):
    high = x.astype(jnp.bfloat16)
    low = (x - high.astype(jnp.float32)).astype(jnp.bfloat16)
    return jnp.concatenate([high, low], axis=0)


def folded(x):
    half = x.shape[0] // 2
    return x[:half] + x[half:]


def lanes(step):
    return pl.ds(pl.multiple_of(step * CHUNK, CHUNK), CHUNK)


def local_call(kernel, shapes, flops, *operands):
    whole = pl.BlockSpec(memory_space=pltpu.VMEM)
    moved = sum(x.size * x.dtype.itemsize for x in operands)
    single = not isinstance(shapes, (list, tuple))
    return pl.pallas_call(
        kernel,
        out_shape=shapes,
        in_specs=[whole] * len(operands),
        out_specs=whole if single else [whole] * len(shapes),
        cost_estimate=pl.CostEstimate(flops=flops, bytes_accessed=moved, transcendentals=0),
        compiler_params=pltpu.CompilerParams(vmem_limit_bytes=24 << 20),
    )(*operands)


def product_kernel(z_ref, half_ref, sums_ref):
    def step(i, total):
        terms = two_terms(z_ref[:, lanes(i)])
        return total + lax.dot_general(
            terms, half_ref[:, lanes(i)], ROWS_BY_LANES, preferred_element_type=jnp.float32
        )

    rows, depth = z_ref.shape
    start = jnp.zeros((2 * rows, half_ref.shape[0]), jnp.float32)
    sums_ref[...] = folded(lax.fori_loop(0, depth // CHUNK, step, start))


def second_product_kernel(z_ref, half_ref, before_ref, sums_ref):
    width = half_ref.shape[0]
    sums_ref[:, :width] = before_ref[...]
    product_kernel(z_ref, half_ref, sums_ref.at[:, width:])


def joined(refs, i):
    return jnp.concatenate([ref[:, lanes(i)] for ref in refs], axis=0)


def step_kernel(z_ref, image_ref, *refs):
    *used_refs, next_ref, new_ref, sums_ref = refs
    image = two_terms(image_ref[...])

    def step(i, total):
        change = jnp.dot(image, joined(used_refs, i), preferred_element_type=jnp.float32)
        current = z_ref[:, lanes(i)] - folded(change)
        new_ref[:, lanes(i)] = current
        return total + lax.dot_general(
            two_terms(current), next_ref[:, lanes(i)], ROWS_BY_LANES, preferred_element_type=jnp.float32
        )

    rows, depth = z_ref.shape
    start = jnp.zeros((2 * rows, next_ref.shape[0]), jnp.float32)
    sums_ref[...] = folded(lax.fori_loop(0, depth // CHUNK, step, start))


def last_kernel(z_ref, image_ref, used_ref, result_ref):
    image = two_terms(image_ref[...])

    def step(i, carry):
        change = jnp.dot(image, used_ref[:, lanes(i)], preferred_element_type=jnp.float32)
        result_ref[lanes(i), :] = (z_ref[:, lanes(i)] - folded(change)).T
        return carry

    lax.fori_loop(0, z_ref.shape[1] // CHUNK, step, 0)


def share_kernel(parts_ref, tri_ref, copies_ref):
    devices = parts_ref.shape[0]
    total = parts_ref[0]
    for device in range(1, devices):
        total = total + parts_ref[device]
    image = lax.dot_general(
        total,
        tri_ref[...],
        ROWS_BY_LANES,
        precision=lax.Precision.HIGHEST,
        preferred_element_type=jnp.float32,
    )
    for device in range(devices):
        copies_ref[device] = image


def share_copies(sums, tri_factor, axis):
    devices = lax.axis_size(axis)
    columns, size = sums.shape
    shape = jax.ShapeDtypeStruct((devices, columns // devices, size), jnp.float32)
    arrived = exchange(sums.reshape(shape.shape), axis)
    flops = 2 * columns // devices * size * size
    return local_call(share_kernel, shape, flops, arrived, tri_factor)


def after(x, *earlier):
    return lax.optimization_barrier((x, *earlier))[0]


def reordered(tri_factor, wanted):
    size = tri_factor.shape[0]
    source = lax.broadcasted_iota(jnp.int32, (size, size), 1)
    choose = (wanted == source).astype(jnp.float32)
    turned = jnp.dot(choose, tri_factor, precision=lax.Precision.HIGHEST)
    return lax.dot_general(turned, choose, ROWS_BY_LANES, precision=lax.Precision.HIGHEST)


def on_device(vectors, reflectors, tau_diag, coupling):
    count, each, rows = reflectors.shape
    high_axis, low_axis, core_axis = PCOL
    wide, deep = lax.axis_size(high_axis), lax.axis_size(low_axis)
    core = lax.axis_index(core_axis)
    last = count - 1
    half = wide * deep * each
    columns = vectors.shape[1]

    early = copy_for_each(reflectors[:last], low_axis, deep)
    early = early.transpose(1, 0, 2, 3).reshape(last, deep * each, rows)
    later = lax.all_gather(early, (high_axis, core_axis), axis=0, tiled=False)

    start = after(reflectors[last], early)
    first = copy_for_each(start, (high_axis, low_axis), wide * deep).reshape(half, rows)
    partner = from_partner(first)

    place = lax.broadcasted_iota(jnp.int32, (2 * half, 2 * half), 0)
    parity = jnp.where(place // half == 0, core, 1 - core)
    rest = place % half
    alone = (rest // each * 2 + parity) * each + rest % each
    spot, inner = place // each, place % each
    high, mid, low = spot // (2 * deep), spot // deep % 2, spot % deep
    together = ((high * deep + low) * 2 + mid) * each + inner

    def factor(position):
        tri_factor = jnp.diag(tau_diag[position]) + jnp.triu(coupling[position], 1)
        return reordered(tri_factor, alone if position == last else together)

    factors = [factor(position) for position in range(count)]
    current = after(vectors.T, *factors)
    pass_flops = 4 * columns * half * rows
    sums_shape = jax.ShapeDtypeStruct((columns, 2 * half), jnp.float32)
    own_shape = jax.ShapeDtypeStruct((columns, half), jnp.float32)
    z_shape = jax.ShapeDtypeStruct(current.shape, jnp.float32)
    sums = local_call(product_kernel, own_shape, pass_flops, current, first)
    sums = local_call(second_product_kernel, sums_shape, pass_flops, current, partner, sums)

    panels = None
    used = [first, partner]
    for k in range(last, -1, -1):
        copies = share_copies(sums, factors[k], "prow")
        if panels is None:
            gathered = after(later, copies)
            panels = [gathered[:, p].reshape(2 * half, rows) for p in range(last)]
        image = exchange(copies, "prow").reshape(columns, 2 * half)
        if k > 0:
            following = panels[k - 1]
            current, sums = local_call(
                step_kernel, [z_shape, sums_shape], 4 * pass_flops, current, image, *used, following
            )
            used = [following]
    result = jax.ShapeDtypeStruct(vectors.shape, jnp.float32)
    return local_call(last_kernel, result, 2 * pass_flops, current, image, *used)


def solution(mesh):
    finer = Mesh(
        mesh.devices.reshape(mesh.shape["prow"], 8, 4, 2), ("prow", "pcol_0", "pcol_1", "pcol_2")
    )
    placed = (P("prow", PCOL), P(None, PCOL, "prow"), P(), P())
    return jax.shard_map(
        on_device, mesh=finer, in_specs=placed, out_specs=P("prow", PCOL), check_vma=False
    )
```

```python
import jax
import jax.numpy as jnp
from jax import lax
from jax.experimental import pallas as pl
from jax.experimental.pallas import tpu as pltpu
from jax.sharding import Mesh
from jax.sharding import PartitionSpec as P


PCOL = ("pcol_0", "pcol_1", "pcol_2")
CHUNK = 512
ROWS_BY_LANES = (((1,), (1,)), ((), ()))


def exchange(parts, axis):
    return lax.all_to_all(parts, axis, split_axis=0, concat_axis=0, tiled=True)


def copy_for_each(x, axis, devices):
    return exchange(jnp.broadcast_to(x, (devices, *x.shape)), axis)


def from_partner(x):
    return lax.ppermute(x, "pcol_2", [(0, 1), (1, 0)])


def shifted(x, axis, by):
    devices = lax.axis_size(axis)
    return lax.ppermute(x, axis, [(i, (i + by) % devices) for i in range(devices)])


def after(x, *earlier):
    return lax.optimization_barrier((x, *earlier))[0]


def two_terms(x):
    high = x.astype(jnp.bfloat16)
    low = (x - high.astype(jnp.float32)).astype(jnp.bfloat16)
    return jnp.concatenate([high, low], axis=0)


def lanes(step):
    return pl.ds(pl.multiple_of(step * CHUNK, CHUNK), CHUNK)


def local_call(kernel, shapes, flops, *operands, scratch=()):
    whole = pl.BlockSpec(memory_space=pltpu.VMEM)
    moved = sum(x.size * x.dtype.itemsize for x in operands)
    single = not isinstance(shapes, (list, tuple))
    return pl.pallas_call(
        kernel,
        out_shape=shapes,
        in_specs=[whole] * len(operands),
        out_specs=whole if single else [whole] * len(shapes),
        scratch_shapes=scratch,
        cost_estimate=pl.CostEstimate(flops=flops, bytes_accessed=moved, transcendentals=0),
        compiler_params=pltpu.CompilerParams(vmem_limit_bytes=24 << 20),
    )(*operands)


def products(half_ref, terms_ref):
    both = lax.dot_general(
        half_ref[...], terms_ref[...], ROWS_BY_LANES, preferred_element_type=jnp.float32
    )
    columns = both.shape[1] // 2
    return both[:, :columns] + both[:, columns:]


def split_kernel(z_ref, turned_ref, terms_ref):
    def step(i, carry):
        turned = z_ref[lanes(i), :].T
        turned_ref[:, lanes(i)] = turned
        terms_ref[:, lanes(i)] = two_terms(turned)
        return carry

    lax.fori_loop(0, z_ref.shape[0] // CHUNK, step, 0)


def first_kernel(terms_ref, half_ref, sums_ref):
    sums_ref[...] = products(half_ref, terms_ref)


def second_kernel(terms_ref, half_ref, before_ref, sums_ref):
    size = before_ref.shape[0]
    sums_ref[:size, :] = before_ref[...]
    sums_ref[size:, :] = products(half_ref, terms_ref)


def image_terms(tri_ref, total_ref):
    image = jnp.dot(
        tri_ref[...], total_ref[...], precision=lax.Precision.HIGHEST, preferred_element_type=jnp.float32
    )
    return two_terms(image.T)


def changed(z_ref, image, own_ref, other_ref, i):
    used = jnp.concatenate([own_ref[:, lanes(i)], other_ref[:, lanes(i)]], axis=0)
    change = jnp.dot(image, used, preferred_element_type=jnp.float32)
    rows = z_ref.shape[0]
    return z_ref[:, lanes(i)] - (change[:rows] + change[rows:])


def step_kernel(
    z_ref, tri_ref, total_ref, own_ref, other_ref, next_own_ref, next_other_ref, new_ref, sums_ref, terms_ref
):
    image = image_terms(tri_ref, total_ref)

    def step(i, carry):
        current = changed(z_ref, image, own_ref, other_ref, i)
        new_ref[:, lanes(i)] = current
        terms_ref[:, lanes(i)] = two_terms(current)
        return carry

    lax.fori_loop(0, z_ref.shape[1] // CHUNK, step, 0)
    size = next_own_ref.shape[0]
    sums_ref[:size, :] = products(next_own_ref, terms_ref)
    sums_ref[size:, :] = products(next_other_ref, terms_ref)


def last_kernel(z_ref, tri_ref, total_ref, own_ref, other_ref, result_ref):
    image = image_terms(tri_ref, total_ref)

    def step(i, carry):
        result_ref[lanes(i), :] = changed(z_ref, image, own_ref, other_ref, i).T
        return carry

    lax.fori_loop(0, z_ref.shape[1] // CHUNK, step, 0)


def share_kernel(parts_ref, copies_ref):
    devices = parts_ref.shape[0]
    total = parts_ref[0]
    for device in range(1, devices):
        total = total + parts_ref[device]
    for device in range(devices):
        copies_ref[device] = total


def reordered(tri_factor, wanted):
    size = tri_factor.shape[0]
    source = lax.broadcasted_iota(jnp.int32, (size, size), 1)
    choose = (wanted == source).astype(jnp.float32)
    turned = jnp.dot(choose, tri_factor, precision=lax.Precision.HIGHEST)
    return lax.dot_general(turned, choose, ROWS_BY_LANES, precision=lax.Precision.HIGHEST)


def on_device(vectors, reflectors, tau_diag, coupling):
    count, each, rows = reflectors.shape
    high_axis, low_axis, core_axis = PCOL
    wide, deep = lax.axis_size(high_axis), lax.axis_size(low_axis)
    core, low = lax.axis_index(core_axis), lax.axis_index(low_axis)
    last = count - 1
    group = wide * each
    half = deep * group
    columns = vectors.shape[1]
    f32 = jnp.float32

    place = lax.broadcasted_iota(jnp.int32, (2 * half, 2 * half), 0)
    parity = jnp.where(place // half == 0, core, 1 - core)
    piece, spot, inner = place % half // group, place % group // each, place % each

    def factor(position):
        tri_factor = jnp.diag(tau_diag[position]) + jnp.triu(coupling[position], 1)
        offset = jnp.where(piece == 1, deep - 1, jnp.where(piece == 2, 1, jnp.where(piece == 3, 2, 0)))
        source = piece if position == last else (low + offset) % deep
        return reordered(tri_factor, ((spot * deep + source) * 2 + parity) * each + inner)

    factors = [factor(position) for position in range(count)]
    z_shape = jax.ShapeDtypeStruct((columns, rows), f32)
    terms_shape = jax.ShapeDtypeStruct((2 * columns, rows), jnp.bfloat16)
    current, terms = local_call(split_kernel, [z_shape, terms_shape], 1 << 24, vectors)

    def along_high(reflectors):
        arrived = copy_for_each(reflectors, high_axis, wide)
        return [arrived[:, k].reshape(group, rows) for k in range(reflectors.shape[0])]

    groups = {}
    groups[last - 1], groups[last] = along_high(reflectors[last - 1 :])
    start = after(groups[last], current, terms, *factors)
    first = copy_for_each(start, low_axis, deep).reshape(half, rows)
    groups[0], groups[1] = along_high(after(reflectors[: last - 1], first))
    partner = from_partner(first)

    pass_flops = 4 * columns * half * rows
    sums_shape = jax.ShapeDtypeStruct((2 * half, columns), f32)
    own_shape = jax.ShapeDtypeStruct((half, columns), f32)
    own_sums = local_call(first_kernel, own_shape, pass_flops, terms, first)
    sums = local_call(second_kernel, sums_shape, pass_flops, terms, partner, own_sums)
    sums = after(sums, groups[0], groups[1])

    def along_low(position, earlier):
        x = after(groups[position], earlier)
        pieces = [x]
        for by in (1, -1, 2):
            pieces.append(shifted(x, low_axis, by))
        return pieces

    devices = lax.axis_size("prow")
    parts_shape = jax.ShapeDtypeStruct((devices, 2 * half // devices, columns), f32)
    sent = {last - 1: along_low(last - 1, first)}
    used = (first, partner)
    for k in range(last, -1, -1):
        if k > 1:
            sent[k - 2] = along_low(k - 2, sums)
        if k > 0:
            own = jnp.concatenate(lax.optimization_barrier((*sent[k - 1], sums))[:-1])
        arrived = exchange(sums.reshape(parts_shape.shape), "prow")
        copies = local_call(share_kernel, parts_shape, 1 << 20, arrived)
        if k > 0:
            following = (own, from_partner(after(own, copies)))
        total = exchange(copies, "prow").reshape(2 * half, columns)
        if k > 0:
            current, sums = local_call(
                step_kernel,
                [z_shape, sums_shape],
                4 * pass_flops,
                current,
                factors[k],
                total,
                *used,
                *following,
                scratch=[pltpu.VMEM(terms_shape.shape, jnp.bfloat16)],
            )
            used = following
    result = jax.ShapeDtypeStruct(vectors.shape, f32)
    return local_call(last_kernel, result, 2 * pass_flops, current, factors[0], total, *used)


def solution(mesh):
    finer = Mesh(
        mesh.devices.reshape(mesh.shape["prow"], 8, 4, 2), ("prow", "pcol_0", "pcol_1", "pcol_2")
    )
    placed = (P("prow", PCOL), P(None, PCOL, "prow"), P(), P())

    return jax.shard_map(
        on_device, mesh=finer, in_specs=placed, out_specs=P("prow", PCOL), check_vma=False
    )
```

```python
import functools

import jax
import jax.numpy as jnp
from jax import lax
from jax.experimental import pallas as pl
from jax.experimental.pallas import tpu as pltpu
from jax.sharding import Mesh
from jax.sharding import PartitionSpec as P

PCOL = ("pcol_0", "pcol_1", "pcol_2")
CHUNK = 512
ROWS_BY_LANES = (((1,), (1,)), ((), ()))


def exchange(parts, axis):
    return lax.all_to_all(parts, axis, split_axis=0, concat_axis=0, tiled=True)


def copy_for_each(x, axis, devices):
    return exchange(jnp.broadcast_to(x, (devices, *x.shape)), axis)


def from_partner(x):
    return lax.ppermute(x, "pcol_2", [(0, 1), (1, 0)])


def two_terms(x):
    high = x.astype(jnp.bfloat16)
    low = (x - high.astype(jnp.float32)).astype(jnp.bfloat16)
    return jnp.concatenate([high, low], axis=0)


def folded(x):
    half = x.shape[0] // 2
    return x[:half] + x[half:]


def lanes(step):
    return pl.ds(pl.multiple_of(step * CHUNK, CHUNK), CHUNK)


def local_call(kernel, shapes, flops, *operands, scratch=()):
    whole = pl.BlockSpec(memory_space=pltpu.VMEM)
    moved = sum(x.size * x.dtype.itemsize for x in operands)
    single = not isinstance(shapes, (list, tuple))
    return pl.pallas_call(
        kernel,
        out_shape=shapes,
        in_specs=[whole] * len(operands),
        out_specs=whole if single else [whole] * len(shapes),
        scratch_shapes=scratch,
        cost_estimate=pl.CostEstimate(flops=flops, bytes_accessed=moved, transcendentals=0),
        compiler_params=pltpu.CompilerParams(vmem_limit_bytes=24 << 20),
    )(*operands)


def products(half_ref, terms_ref):
    both = lax.dot_general(
        half_ref[...], terms_ref[...], ROWS_BY_LANES, preferred_element_type=jnp.float32
    )
    columns = both.shape[1] // 2
    return (both[:, :columns] + both[:, columns:]).T


def split_kernel(z_ref, turned_ref, terms_ref):
    def step(i, carry):
        turned = z_ref[lanes(i), :].T
        turned_ref[:, lanes(i)] = turned
        terms_ref[:, lanes(i)] = two_terms(turned)
        return carry

    lax.fori_loop(0, z_ref.shape[0] // CHUNK, step, 0)


def first_kernel(terms_ref, half_ref, sums_ref):
    sums_ref[...] = products(half_ref, terms_ref)


def second_kernel(terms_ref, half_ref, before_ref, sums_ref):
    size = before_ref.shape[1]
    sums_ref[:, :size] = before_ref[...]
    sums_ref[:, size:] = products(half_ref, terms_ref)


def joined(refs, i):
    return jnp.concatenate([ref[:, lanes(i)] for ref in refs], axis=0)


def step_kernel(z_ref, image_ref, *refs):
    *used_refs, next_ref, new_ref, sums_ref, terms_ref = refs
    image = two_terms(image_ref[...])

    def step(i, carry):
        change = jnp.dot(image, joined(used_refs, i), preferred_element_type=jnp.float32)
        current = z_ref[:, lanes(i)] - folded(change)
        new_ref[:, lanes(i)] = current
        terms_ref[:, lanes(i)] = two_terms(current)
        return carry

    lax.fori_loop(0, z_ref.shape[1] // CHUNK, step, 0)
    sums_ref[...] = products(next_ref, terms_ref)


def last_kernel(z_ref, image_ref, used_ref, result_ref):
    image = two_terms(image_ref[...])

    def step(i, carry):
        change = jnp.dot(image, used_ref[:, lanes(i)], preferred_element_type=jnp.float32)
        result_ref[lanes(i), :] = (z_ref[:, lanes(i)] - folded(change)).T
        return carry

    lax.fori_loop(0, z_ref.shape[1] // CHUNK, step, 0)


def share_kernel(parts_ref, tri_ref, copies_ref):
    devices = parts_ref.shape[0]
    total = parts_ref[0]
    for device in range(1, devices):
        total = total + parts_ref[device]
    image = lax.dot_general(
        total,
        tri_ref[...],
        ROWS_BY_LANES,
        precision=lax.Precision.HIGHEST,
        preferred_element_type=jnp.float32,
    )
    for device in range(devices):
        copies_ref[device] = image


def share_copies(sums, tri_factor, axis):
    devices = lax.axis_size(axis)
    columns, size = sums.shape
    shape = jax.ShapeDtypeStruct((devices, columns // devices, size), jnp.float32)
    arrived = exchange(sums.reshape(shape.shape), axis)
    flops = 2 * columns // devices * size * size
    return local_call(share_kernel, shape, flops, arrived, tri_factor)


def after(x, *earlier):
    return lax.optimization_barrier((x, *earlier))[0]


def reordered(tri_factor, wanted):
    size = tri_factor.shape[0]
    source = lax.broadcasted_iota(jnp.int32, (size, size), 1)
    choose = (wanted == source).astype(jnp.float32)
    turned = jnp.dot(choose, tri_factor, precision=lax.Precision.HIGHEST)
    return lax.dot_general(turned, choose, ROWS_BY_LANES, precision=lax.Precision.HIGHEST)


def on_device(vectors, reflectors, tau_diag, coupling):
    count, each, rows = reflectors.shape
    high_axis, low_axis, core_axis = PCOL
    wide, deep = lax.axis_size(high_axis), lax.axis_size(low_axis)
    core = lax.axis_index(core_axis)
    last = count - 1
    half = wide * deep * each
    columns = vectors.shape[1]

    early = copy_for_each(reflectors[:last], low_axis, deep)
    early = early.transpose(1, 0, 2, 3).reshape(last, deep * each, rows)
    later = lax.all_gather(early, (high_axis, core_axis), axis=0, tiled=False)

    group = copy_for_each(after(reflectors[last], early), high_axis, wide).reshape(wide * each, rows)

    place = lax.broadcasted_iota(jnp.int32, (2 * half, 2 * half), 0)
    parity = jnp.where(place // half == 0, core, 1 - core)
    across, along = place % half // (wide * each), place % (wide * each) // each
    alone = ((along * deep + across) * 2 + parity) * each + place % each
    spot, inner = place // each, place % each
    high, mid, low = spot // (2 * deep), spot // deep % 2, spot % deep
    together = ((high * deep + low) * 2 + mid) * each + inner

    def factor(position):
        tri_factor = jnp.diag(tau_diag[position]) + jnp.triu(coupling[position], 1)
        return reordered(tri_factor, alone if position == last else together)

    factors = [factor(position) for position in range(count)]
    pass_flops = 4 * columns * half * rows
    sums_shape = jax.ShapeDtypeStruct((columns, 2 * half), jnp.float32)
    own_shape = jax.ShapeDtypeStruct((columns, half), jnp.float32)
    z_shape = jax.ShapeDtypeStruct((columns, rows), jnp.float32)
    terms_shape = jax.ShapeDtypeStruct((2 * columns, rows), jnp.bfloat16)
    current, terms = local_call(split_kernel, [z_shape, terms_shape], 1 << 24, vectors)
    start = after(group, current, terms, *factors)
    first = copy_for_each(start, low_axis, deep).reshape(half, rows)
    partner = from_partner(first)
    sums = local_call(first_kernel, own_shape, pass_flops, terms, first)
    sums = local_call(second_kernel, sums_shape, pass_flops, terms, partner, sums)

    panels = None
    used = [first, partner]
    for k in range(last, -1, -1):
        copies = share_copies(sums, factors[k], "prow")
        if panels is None:
            gathered = after(later, copies)
            panels = [gathered[:, p].reshape(2 * half, rows) for p in range(last)]
        image = exchange(copies, "prow").reshape(columns, 2 * half)
        if k > 0:
            following = panels[k - 1]
            current, sums = local_call(
                step_kernel,
                [z_shape, sums_shape],
                4 * pass_flops,
                current,
                image,
                *used,
                following,
                scratch=[pltpu.VMEM(terms_shape.shape, jnp.bfloat16)],
            )
            used = [following]
    result = jax.ShapeDtypeStruct(vectors.shape, jnp.float32)
    return local_call(last_kernel, result, 2 * pass_flops, current, image, *used)


def solution(mesh):
    finer = Mesh(
        mesh.devices.reshape(mesh.shape["prow"], 8, 4, 2), ("prow", "pcol_0", "pcol_1", "pcol_2")
    )
    placed = (P("prow", PCOL), P(None, PCOL, "prow"), P(), P())
    return jax.shard_map(
        on_device, mesh=finer, in_specs=placed, out_specs=P("prow", PCOL), check_vma=False
    )
```

```python
import functools

import jax
import jax.numpy as jnp
from jax import lax
from jax.experimental import pallas as pl
from jax.experimental.pallas import tpu as pltpu
from jax.sharding import Mesh
from jax.sharding import PartitionSpec as P

PCOL = ("pcol_0", "pcol_1", "pcol_2")
CHUNK = 1024
F32 = jnp.float32
BF16 = jnp.bfloat16
ROWS_BY_LANES = (((1,), (1,)), ((), ()))
LIMIT = 24 << 20


def exchange(parts, axis):
    return lax.all_to_all(parts, axis, split_axis=0, concat_axis=0, tiled=True)


def copy_for_each(x, axis, devices):
    return exchange(jnp.broadcast_to(x, (devices, *x.shape)), axis)


def from_partner(x):
    return lax.ppermute(x, "pcol_2", [(0, 1), (1, 0)])


def after(x, *earlier):
    return lax.optimization_barrier((x, *earlier))[0]


def two_terms(x):
    high = x.astype(BF16)
    low = (x - high.astype(F32)).astype(BF16)
    return jnp.concatenate([high, low], axis=0)


def folded(x):
    half = x.shape[0] // 2
    return x[:half] + x[half:]


def cost(flops, *operands):
    moved = sum(x.size * x.dtype.itemsize for x in operands)
    return pl.CostEstimate(flops=flops, bytes_accessed=moved, transcendentals=0)


def whole(memory_space=pltpu.VMEM):
    return pl.BlockSpec(memory_space=memory_space)


def local_call(kernel, shapes, flops, *operands, scalars=0):
    single = not isinstance(shapes, (list, tuple))
    return pl.pallas_call(
        kernel,
        out_shape=shapes,
        in_specs=[whole(pltpu.SMEM)] * scalars + [whole()] * (len(operands) - scalars),
        out_specs=whole() if single else [whole()] * len(shapes),
        cost_estimate=cost(flops, *operands),
        compiler_params=pltpu.CompilerParams(vmem_limit_bytes=LIMIT),
    )(*operands)


def fixed(*shape):
    return pl.BlockSpec(shape, lambda i: (0,) * len(shape))


def by_lanes(rows):
    return pl.BlockSpec((rows, CHUNK), lambda i: (0, i))


def panel_of(gathered, position):
    owners, _, inner, _ = gathered.shape
    return pl.BlockSpec((owners, None, inner, CHUNK), lambda i: (0, position, 0, i))


def streamed_call(kernel, shapes, in_specs, out_specs, scratch, flops, *operands):
    return pl.pallas_call(
        kernel,
        grid=(4096 // CHUNK,),
        out_shape=shapes,
        in_specs=in_specs,
        out_specs=out_specs,
        scratch_shapes=scratch,
        cost_estimate=cost(flops, *operands),
        compiler_params=pltpu.CompilerParams(
            vmem_limit_bytes=LIMIT, dimension_semantics=("arbitrary",)
        ),
    )(*operands)


def rows_of(ref):
    owners, inner, width = ref.shape
    return ref[...].reshape(owners * inner, width)


def products(reflectors, terms):
    return lax.dot_general(reflectors, terms, ROWS_BY_LANES, preferred_element_type=F32)


def settled(both):
    columns = both.shape[1] // 2
    return (both[:, :columns] + both[:, columns:]).T


def split_kernel(z_ref, turned_ref, terms_ref):
    for i in range(z_ref.shape[0] // CHUNK):
        part = slice(i * CHUNK, (i + 1) * CHUNK)
        turned = z_ref[part, :].T
        turned_ref[:, part] = turned
        terms_ref[:, part] = two_terms(turned)


def first_kernel(terms_ref, half_ref, sums_ref):
    sums_ref[...] = settled(products(half_ref[...], terms_ref[...]))


def second_kernel(terms_ref, half_ref, before_ref, sums_ref):
    size = before_ref.shape[1]
    sums_ref[:, :size] = before_ref[...]
    sums_ref[:, size:] = settled(products(half_ref[...], terms_ref[...]))


def gram_kernel(core_ref, half_ref, other_ref, gram_ref):
    @pl.when(pl.program_id(0) == 0)
    def _():
        gram_ref[...] = jnp.zeros_like(gram_ref)

    gram_ref[...] += products(rows_of(half_ref), rows_of(other_ref))


def updated(z_ref, image, used):
    change = jnp.dot(two_terms(image), used, preferred_element_type=F32)
    return z_ref[...] - folded(change)


def accumulated(total_ref, part):
    @pl.when(pl.program_id(0) == 0)
    def _():
        total_ref[...] = part

    @pl.when(pl.program_id(0) > 0)
    def _():
        total_ref[...] += part


def ended():
    return pl.program_id(0) == pl.num_programs(0) - 1


def step_kernel(z_ref, image_ref, own_ref, partner_ref, next_ref, gram_ref, new_ref, parts_ref, total_ref):
    used = jnp.concatenate([own_ref[...], partner_ref[...]], axis=0)
    current = updated(z_ref, image_ref[...], used)
    new_ref[...] = current
    accumulated(total_ref, products(rows_of(next_ref), two_terms(current)))

    @pl.when(ended())
    def _():
        devices, both, size = parts_ref.shape
        parts_ref[:, : both // 2, :] = settled(total_ref[...]).reshape(devices, both // 2, size)
        parts_ref[:, both // 2 :, :] = gram_ref[...].reshape(devices, both // 2, size)


def pair_kernel(z_ref, copies_ref, used_ref, high_ref, low_ref, new_ref, sums_ref, total_ref):
    devices, both, size = copies_ref.shape
    image = copies_ref[:, : both // 2, :].reshape(devices * both // 2, size)
    current = updated(z_ref, image, rows_of(used_ref))
    new_ref[...] = current
    following = jnp.concatenate([rows_of(high_ref), rows_of(low_ref)], axis=0)
    accumulated(total_ref, products(following, two_terms(current)))

    @pl.when(ended())
    def _():
        sums_ref[...] = settled(total_ref[...])


def last_kernel(z_ref, image_ref, high_ref, low_ref, result_ref):
    used = jnp.concatenate([rows_of(high_ref), rows_of(low_ref)], axis=0)
    result_ref[...] = updated(z_ref, image_ref[...], used).T


def applied(x, matrix):
    return lax.dot_general(
        x, matrix, ROWS_BY_LANES, precision=lax.Precision.HIGHEST, preferred_element_type=F32
    )


def summed(parts_ref):
    total = parts_ref[0]
    for device in range(1, parts_ref.shape[0]):
        total = total + parts_ref[device]
    return total


def share_kernel(parts_ref, tri_ref, copies_ref):
    image = applied(summed(parts_ref), tri_ref[...])
    for device in range(parts_ref.shape[0]):
        copies_ref[device] = image


def gram_share_kernel(parts_ref, tri_ref, copies_ref):
    total = summed(parts_ref)
    rows = total.shape[0] // 2
    image = applied(total[:rows], tri_ref[...])
    for device in range(parts_ref.shape[0]):
        copies_ref[device, :rows] = image
        copies_ref[device, rows:] = total[rows:]


def pair_share_kernel(parts_ref, high_ref, low_ref, gram_ref, copies_ref):
    total = summed(parts_ref)
    size = total.shape[1] // 2
    high = applied(total[:, :size], high_ref[...])
    low = applied(total[:, size:] - applied(high, gram_ref[...]), low_ref[...])
    for device in range(parts_ref.shape[0]):
        copies_ref[device, :, :size] = high
        copies_ref[device, :, size:] = low


def factor_kernel(wide, deep, each, core_ref, tau_ref, coupling_ref, *factor_refs):
    size = tau_ref.shape[1]
    row = lax.broadcasted_iota(jnp.int32, (size, size), 0)
    column = lax.broadcasted_iota(jnp.int32, (size, size), 1)
    spot, inner = row // each, row % each
    high, mid, low = spot // (2 * deep), spot // deep % 2, spot % deep
    together = ((high * deep + low) * 2 + mid) * each + inner
    core = core_ref[0]
    part, rest = row // (size // 2), row % (size // 2)
    parity = jnp.where(part == 0, core, 1 - core)
    across, along = rest // (wide * each), rest % (wide * each) // each
    alone = ((along * deep + across) * 2 + parity) * each + inner
    for position, factor_ref in enumerate(factor_refs):
        wanted = alone if position == len(factor_refs) - 1 else together
        choose = (wanted == column).astype(F32)
        upper = jnp.where(column > row, coupling_ref[position], 0.0)
        factor = jnp.where(column == row, tau_ref[position : position + 1, :], upper)
        turned = jnp.dot(choose, factor, precision=lax.Precision.HIGHEST, preferred_element_type=F32)
        factor_ref[...] = applied(turned, choose)


def on_device(vectors, reflectors, tau_diag, coupling):
    count, each, rows = reflectors.shape
    high_axis, low_axis, core_axis = PCOL
    wide, deep = lax.axis_size(high_axis), lax.axis_size(low_axis)
    devices = lax.axis_size("prow")
    core = lax.axis_index(core_axis)
    last = count - 1
    half = wide * deep * each
    size = 2 * half
    columns = vectors.shape[1]
    share = columns // devices

    def shape(*lengths, dtype=F32):
        return jax.ShapeDtypeStruct(lengths, dtype)

    early = copy_for_each(reflectors[:last], low_axis, deep)
    early = early.transpose(1, 0, 2, 3).reshape(last, deep * each, rows)
    later = lax.all_gather(early, (high_axis, core_axis), axis=0, tiled=False)

    group = copy_for_each(after(reflectors[last], early), high_axis, wide).reshape(wide * each, rows)

    where_core = core.astype(jnp.int32).reshape(1)
    factors = local_call(
        functools.partial(factor_kernel, wide, deep, each),
        [shape(size, size)] * count,
        count * 24 * size**3,
        where_core,
        tau_diag,
        coupling,
        scalars=1,
    )
    current, terms = local_call(
        split_kernel, [shape(columns, rows), shape(2 * columns, rows, dtype=BF16)], 1 << 24, vectors
    )
    start = after(group, current, terms, *factors)
    first = copy_for_each(start, low_axis, deep).reshape(half, rows)
    partner = from_partner(first)

    once = 4 * columns * half * rows
    sums = local_call(first_kernel, shape(columns, half), once, terms, first)
    sums = local_call(second_kernel, shape(columns, size), once, terms, partner, sums)
    arrived = exchange(sums.reshape(devices, share, size), "prow")
    copies = local_call(share_kernel, shape(devices, share, size), 1 << 24, arrived, factors[3])

    gathered = after(later, copies)
    owners, _, inner, _ = gathered.shape
    gram_half = pl.pallas_call(
        gram_kernel,
        grid_spec=pltpu.PrefetchScalarGridSpec(
            num_scalar_prefetch=1,
            grid=(rows // CHUNK,),
            in_specs=[
                pl.BlockSpec((owners // 2, None, inner, CHUNK), lambda i, core: (core[0], 0, 0, i)),
                pl.BlockSpec((owners, None, inner, CHUNK), lambda i, core: (0, 1, 0, i)),
            ],
            out_specs=pl.BlockSpec((half, size), lambda i, core: (0, 0)),
        ),
        out_shape=shape(half, size),
        cost_estimate=cost(2 * half * size * rows, gathered),
        compiler_params=pltpu.CompilerParams(
            vmem_limit_bytes=LIMIT, dimension_semantics=("arbitrary",)
        ),
    )(where_core, gathered, gathered)

    image = exchange(copies, "prow").reshape(columns, size)
    current, parts = streamed_call(
        step_kernel,
        [shape(columns, rows), shape(devices, 2 * share, size)],
        [
            by_lanes(columns),
            fixed(columns, size),
            by_lanes(half),
            by_lanes(half),
            panel_of(gathered, 2),
            fixed(half, size),
        ],
        [by_lanes(columns), fixed(devices, 2 * share, size)],
        [pltpu.VMEM((size, 2 * columns), F32)],
        4 * once,
        current,
        image,
        first,
        partner,
        gathered,
        gram_half,
    )
    arrived = exchange(parts, "prow")
    copies = local_call(gram_share_kernel, shape(*parts.shape), 1 << 24, arrived, factors[2])
    copies = exchange(copies, "prow")
    gram_own = copies[:, share:].reshape(half, size)
    gram_other = from_partner(gram_own)
    gram = jnp.where(
        core == 0,
        jnp.concatenate([gram_own, gram_other]),
        jnp.concatenate([gram_other, gram_own]),
    )
    current, sums = streamed_call(
        pair_kernel,
        [shape(columns, rows), shape(columns, 2 * size)],
        [
            by_lanes(columns),
            fixed(devices, 2 * share, size),
            panel_of(gathered, 2),
            panel_of(gathered, 1),
            panel_of(gathered, 0),
        ],
        [by_lanes(columns), fixed(columns, 2 * size)],
        [pltpu.VMEM((2 * size, 2 * columns), F32)],
        6 * once,
        current,
        copies,
        gathered,
        gathered,
        gathered,
    )
    arrived = exchange(sums.reshape(devices, share, 2 * size), "prow")
    copies = local_call(
        pair_share_kernel, shape(*arrived.shape), 1 << 24, arrived, factors[1], factors[0], gram
    )
    image = exchange(copies, "prow").reshape(columns, 2 * size)
    return streamed_call(
        last_kernel,
        shape(*vectors.shape),
        [by_lanes(columns), fixed(columns, 2 * size), panel_of(gathered, 1), panel_of(gathered, 0)],
        pl.BlockSpec((CHUNK, columns), lambda i: (i, 0)),
        [],
        4 * once,
        current,
        image,
        gathered,
        gathered,
    )


def solution(mesh):
    finer = Mesh(
        mesh.devices.reshape(mesh.shape["prow"], 8, 4, 2), ("prow", "pcol_0", "pcol_1", "pcol_2")
    )
    placed = (P("prow", PCOL), P(None, PCOL, "prow"), P(), P())
    return jax.shard_map(
        on_device, mesh=finer, in_specs=placed, out_specs=P("prow", PCOL), check_vma=False
    )
```

```python
import functools

import jax
import jax.numpy as jnp
from jax import lax
from jax.experimental import pallas as pl
from jax.experimental.pallas import tpu as pltpu
from jax.sharding import Mesh
from jax.sharding import PartitionSpec as P

PCOL = ("pcol_0", "pcol_1", "pcol_2")
CHUNK = 1024
PIECE = 512
F32 = jnp.float32
BF16 = jnp.bfloat16
ROWS_BY_LANES = (((1,), (1,)), ((), ()))
LIMIT = 24 << 20
FETCH_LIMIT = 52 << 20
GRAM_LIMIT = 60 << 20


def exchange(parts, axis):
    return lax.all_to_all(parts, axis, split_axis=0, concat_axis=0, tiled=True)


def copy_for_each(x, axis, devices):
    return exchange(jnp.broadcast_to(x, (devices, *x.shape)), axis)


def from_partner(x):
    return lax.ppermute(x, "pcol_2", [(0, 1), (1, 0)])


def after(x, *earlier):
    return lax.optimization_barrier((x, *earlier))[0]


def two_terms(x):
    high = x.astype(BF16)
    low = (x - high.astype(F32)).astype(BF16)
    return jnp.concatenate([high, low], axis=0)


def folded(x):
    half = x.shape[0] // 2
    return x[:half] + x[half:]


def cost(flops, *operands):
    moved = sum(x.size * x.dtype.itemsize for x in operands)
    return pl.CostEstimate(flops=flops, bytes_accessed=moved, transcendentals=0)


def whole(memory_space=pltpu.VMEM):
    return pl.BlockSpec(memory_space=memory_space)


def local_call(kernel, shapes, flops, *operands, scalars=0):
    single = not isinstance(shapes, (list, tuple))
    return pl.pallas_call(
        kernel,
        out_shape=shapes,
        in_specs=[whole(pltpu.SMEM)] * scalars + [whole()] * (len(operands) - scalars),
        out_specs=whole() if single else [whole()] * len(shapes),
        cost_estimate=cost(flops, *operands),
        compiler_params=pltpu.CompilerParams(vmem_limit_bytes=LIMIT),
    )(*operands)


def fetching_call(kernel, shapes, out_spaces, scratch, flops, far, near):
    return pl.pallas_call(
        kernel,
        out_shape=shapes,
        in_specs=[whole(pltpu.HBM)] * len(far) + [whole()] * len(near),
        out_specs=[whole(space) for space in out_spaces],
        scratch_shapes=scratch,
        cost_estimate=cost(flops, *far, *near),
        compiler_params=pltpu.CompilerParams(vmem_limit_bytes=FETCH_LIMIT),
    )(*far, *near)


def rows_of(ref):
    owners, inner, width = ref.shape
    return ref[...].reshape(owners * inner, width)


def products(reflectors, terms):
    return lax.dot_general(reflectors, terms, ROWS_BY_LANES, preferred_element_type=F32)


def settled(both):
    columns = both.shape[1] // 2
    return (both[:, :columns] + both[:, columns:]).T


def split_kernel(z_ref, turned_ref, terms_ref):
    for i in range(z_ref.shape[0] // CHUNK):
        part = slice(i * CHUNK, (i + 1) * CHUNK)
        turned = z_ref[part, :].T
        turned_ref[:, part] = turned
        terms_ref[:, part] = two_terms(turned)


def first_kernel(terms_ref, half_ref, sums_ref):
    sums_ref[...] = settled(products(half_ref[...], terms_ref[...]))


def second_kernel(terms_ref, half_ref, before_ref, sums_ref):
    size = before_ref.shape[1]
    sums_ref[:, :size] = before_ref[...]
    sums_ref[:, size:] = settled(products(half_ref[...], terms_ref[...]))


def gram_kernel(core_ref, half_ref, other_ref, gram_ref):
    @pl.when(pl.program_id(0) == 0)
    def _():
        gram_ref[...] = jnp.zeros_like(gram_ref)

    gram_ref[...] += products(rows_of(half_ref), rows_of(other_ref))


def stretch(i):
    return slice(i * PIECE, (i + 1) * PIECE)


def fetched(sources, buffers, arrivals):
    copies = []
    for i in range(buffers[0].shape[-1] // PIECE):
        row = []
        for k, (source, buffer) in enumerate(zip(sources, buffers)):
            part = (slice(None),) * (len(buffer.shape) - 1) + (pl.ds(i * PIECE, PIECE),)
            row.append(pltpu.make_async_copy(source.at[part], buffer.at[part], arrivals.at[k, i]))
            row[-1].start()
        copies.append(row)
    return copies


def returned(buffer, target, departures, i):
    part = (slice(None), pl.ds(i * PIECE, PIECE))
    return pltpu.make_async_copy(buffer.at[part], target.at[part], departures.at[i])


def piece_of(buffer, i):
    if len(buffer.shape) == 2:
        return buffer[:, stretch(i)]
    owners, inner, _ = buffer.shape
    return buffer[:, :, stretch(i)].reshape(owners * inner, PIECE)


def stacked(buffers, i):
    return jnp.concatenate([piece_of(buffer, i) for buffer in buffers], axis=0)


def advanced(image, sources, z_new, buffers, used, following, total, arrivals, departures):
    z_buffer = buffers[0]
    copies = fetched(sources, buffers, arrivals)
    terms = two_terms(image)
    for i, row in enumerate(copies):
        for copy in row:
            copy.wait()
        change = jnp.dot(terms, stacked(used, i), preferred_element_type=F32)
        current = z_buffer[:, stretch(i)] - folded(change)
        z_buffer[:, stretch(i)] = current
        part = products(stacked(following, i), two_terms(current))
        if i == 0:
            total[...] = part
        else:
            total[...] += part
            returned(z_buffer, z_new, departures, i - 1).start()
    returned(z_buffer, z_new, departures, len(copies) - 1).start()


def drained(z_buffer, z_new, departures):
    for i in range(z_buffer.shape[1] // PIECE):
        returned(z_buffer, z_new, departures, i).wait()


def step_kernel(
    z, own, partner, gathered, image_ref, gram_ref, z_new, parts_ref,
    z_buffer, own_buffer, partner_buffer, next_buffer, total, arrivals, departures,
):
    advanced(
        image_ref[...],
        [z, own, partner, gathered.at[:, 2]],
        z_new,
        [z_buffer, own_buffer, partner_buffer, next_buffer],
        [own_buffer, partner_buffer],
        [next_buffer],
        total,
        arrivals,
        departures,
    )
    devices, both, size = parts_ref.shape
    parts_ref[:, : both // 2, :] = settled(total[...]).reshape(devices, both // 2, size)
    parts_ref[:, both // 2 :, :] = gram_ref[...].reshape(devices, both // 2, size)
    drained(z_buffer, z_new, departures)


def pair_kernel(
    z, gathered, copies_ref, z_new, sums_ref,
    z_buffer, used_buffer, high_buffer, low_buffer, total, arrivals, departures,
):
    devices, both, size = copies_ref.shape
    advanced(
        copies_ref[:, : both // 2, :].reshape(devices * both // 2, size),
        [z, gathered.at[:, 2], gathered.at[:, 1], gathered.at[:, 0]],
        z_new,
        [z_buffer, used_buffer, high_buffer, low_buffer],
        [used_buffer],
        [high_buffer, low_buffer],
        total,
        arrivals,
        departures,
    )
    sums_ref[...] = settled(total[...])
    drained(z_buffer, z_new, departures)


def last_kernel(
    z, gathered, image_ref, result, z_buffer, high_buffer, low_buffer, out_buffer, arrivals, departures
):
    buffers = [z_buffer, high_buffer, low_buffer]
    copies = fetched([z, gathered.at[:, 1], gathered.at[:, 0]], buffers, arrivals)
    terms = two_terms(image_ref[...])

    def leaving(i):
        part = pl.ds(i * PIECE, PIECE)
        return pltpu.make_async_copy(out_buffer.at[part, :], result.at[part, :], departures.at[i])

    for i, row in enumerate(copies):
        for copy in row:
            copy.wait()
        change = jnp.dot(terms, stacked(buffers[1:], i), preferred_element_type=F32)
        out_buffer[stretch(i), :] = (z_buffer[:, stretch(i)] - folded(change)).T
        if i > 0:
            leaving(i - 1).start()
    leaving(len(copies) - 1).start()
    for i in range(len(copies)):
        leaving(i).wait()


def applied(x, matrix):
    return lax.dot_general(
        x, matrix, ROWS_BY_LANES, precision=lax.Precision.HIGHEST, preferred_element_type=F32
    )


def summed(parts_ref):
    total = parts_ref[0]
    for device in range(1, parts_ref.shape[0]):
        total = total + parts_ref[device]
    return total


def share_kernel(parts_ref, tri_ref, copies_ref):
    image = applied(summed(parts_ref), tri_ref[...])
    for device in range(parts_ref.shape[0]):
        copies_ref[device] = image


def gram_share_kernel(parts_ref, tri_ref, copies_ref):
    total = summed(parts_ref)
    rows = total.shape[0] // 2
    image = applied(total[:rows], tri_ref[...])
    for device in range(parts_ref.shape[0]):
        copies_ref[device, :rows] = image
        copies_ref[device, rows:] = total[rows:]


def pair_share_kernel(parts_ref, high_ref, low_ref, gram_ref, copies_ref):
    total = summed(parts_ref)
    size = total.shape[1] // 2
    high = applied(total[:, :size], high_ref[...])
    low = applied(total[:, size:] - applied(high, gram_ref[...]), low_ref[...])
    for device in range(parts_ref.shape[0]):
        copies_ref[device, :, :size] = high
        copies_ref[device, :, size:] = low


def factor_kernel(wide, deep, each, core_ref, tau_ref, coupling_ref, *factor_refs):
    size = tau_ref.shape[1]
    row = lax.broadcasted_iota(jnp.int32, (size, size), 0)
    column = lax.broadcasted_iota(jnp.int32, (size, size), 1)
    spot, inner = row // each, row % each
    high, mid, low = spot // (2 * deep), spot // deep % 2, spot % deep
    together = ((high * deep + low) * 2 + mid) * each + inner
    core = core_ref[0]
    part, rest = row // (size // 2), row % (size // 2)
    parity = jnp.where(part == 0, core, 1 - core)
    across, along = rest // (wide * each), rest % (wide * each) // each
    alone = ((along * deep + across) * 2 + parity) * each + inner
    for position, factor_ref in enumerate(factor_refs):
        wanted = alone if position == len(factor_refs) - 1 else together
        choose = (wanted == column).astype(F32)
        upper = jnp.where(column > row, coupling_ref[position], 0.0)
        factor = jnp.where(column == row, tau_ref[position : position + 1, :], upper)
        turned = jnp.dot(choose, factor, precision=lax.Precision.HIGHEST, preferred_element_type=F32)
        factor_ref[...] = applied(turned, choose)


def on_device(vectors, reflectors, tau_diag, coupling):
    count, each, rows = reflectors.shape
    high_axis, low_axis, core_axis = PCOL
    wide, deep = lax.axis_size(high_axis), lax.axis_size(low_axis)
    devices = lax.axis_size("prow")
    core = lax.axis_index(core_axis)
    last = count - 1
    half = wide * deep * each
    size = 2 * half
    columns = vectors.shape[1]
    share = columns // devices

    def shape(*lengths, dtype=F32):
        return jax.ShapeDtypeStruct(lengths, dtype)

    hopped = copy_for_each(reflectors[:last], low_axis, deep)
    early = hopped.transpose(1, 0, 2, 3).reshape(last, deep * each, rows)
    later = lax.all_gather(early, (high_axis, core_axis), axis=0, tiled=False)

    group = copy_for_each(after(reflectors[last], hopped), high_axis, wide).reshape(wide * each, rows)

    where_core = core.astype(jnp.int32).reshape(1)
    factors = local_call(
        functools.partial(factor_kernel, wide, deep, each),
        [shape(size, size)] * count,
        count * 24 * size**3,
        where_core,
        tau_diag,
        coupling,
        scalars=1,
    )
    current, terms = local_call(
        split_kernel, [shape(columns, rows), shape(2 * columns, rows, dtype=BF16)], 1 << 24, vectors
    )
    start = after(group, current, terms, *factors)
    first = copy_for_each(start, low_axis, deep).reshape(half, rows)
    partner = from_partner(first)

    once = 4 * columns * half * rows
    sums = local_call(first_kernel, shape(columns, half), once, terms, first)
    sums = local_call(second_kernel, shape(columns, size), once, terms, partner, sums)
    arrived = exchange(sums.reshape(devices, share, size), "prow")
    copies = local_call(share_kernel, shape(devices, share, size), 1 << 24, arrived, factors[3])

    gathered = after(later, copies)
    owners, _, inner, _ = gathered.shape
    gram_half = pl.pallas_call(
        gram_kernel,
        grid_spec=pltpu.PrefetchScalarGridSpec(
            num_scalar_prefetch=1,
            grid=(rows // CHUNK,),
            in_specs=[
                pl.BlockSpec((owners // 2, None, inner, CHUNK), lambda i, core: (core[0], 0, 0, i)),
                pl.BlockSpec((owners, None, inner, CHUNK), lambda i, core: (0, 1, 0, i)),
            ],
            out_specs=pl.BlockSpec((half, size), lambda i, core: (0, 0)),
        ),
        out_shape=shape(half, size),
        cost_estimate=cost(2 * half * size * rows, gathered),
        compiler_params=pltpu.CompilerParams(
            vmem_limit_bytes=GRAM_LIMIT, dimension_semantics=("arbitrary",)
        ),
    )(where_core, gathered, gathered)

    image = exchange(copies, "prow").reshape(columns, size)
    pieces = rows // PIECE
    z_scratch = pltpu.VMEM((columns, rows), F32)
    half_scratch = pltpu.VMEM((half, rows), BF16)
    panel_scratch = pltpu.VMEM((owners, inner, rows), BF16)
    departures = pltpu.SemaphoreType.DMA((pieces,))

    def arrivals(arrays):
        return pltpu.SemaphoreType.DMA((arrays, pieces))

    spaces = [pltpu.HBM, pltpu.VMEM]
    current, parts = fetching_call(
        step_kernel,
        [shape(columns, rows), shape(devices, 2 * share, size)],
        spaces,
        [
            z_scratch, half_scratch, half_scratch, panel_scratch,
            pltpu.VMEM((size, 2 * columns), F32), arrivals(4), departures,
        ],
        4 * once,
        [current, first, partner, gathered],
        [image, gram_half],
    )
    arrived = exchange(parts, "prow")
    copies = local_call(gram_share_kernel, shape(*parts.shape), 1 << 24, arrived, factors[2])
    copies = exchange(copies, "prow")
    gram_own = copies[:, share:].reshape(half, size)
    gram_other = from_partner(gram_own)
    gram = jnp.where(
        core == 0,
        jnp.concatenate([gram_own, gram_other]),
        jnp.concatenate([gram_other, gram_own]),
    )
    current, sums = fetching_call(
        pair_kernel,
        [shape(columns, rows), shape(columns, 2 * size)],
        spaces,
        [
            z_scratch, panel_scratch, panel_scratch, panel_scratch,
            pltpu.VMEM((2 * size, 2 * columns), F32), arrivals(4), departures,
        ],
        6 * once,
        [current, gathered],
        [copies],
    )
    arrived = exchange(sums.reshape(devices, share, 2 * size), "prow")
    copies = local_call(
        pair_share_kernel, shape(*arrived.shape), 1 << 24, arrived, factors[1], factors[0], gram
    )
    image = exchange(copies, "prow").reshape(columns, 2 * size)
    return fetching_call(
        last_kernel,
        [shape(*vectors.shape)],
        [pltpu.HBM],
        [
            z_scratch, panel_scratch, panel_scratch, pltpu.VMEM(vectors.shape, F32),
            arrivals(3), departures,
        ],
        4 * once,
        [current, gathered],
        [image],
    )[0]


def solution(mesh):
    finer = Mesh(
        mesh.devices.reshape(mesh.shape["prow"], 8, 4, 2), ("prow", "pcol_0", "pcol_1", "pcol_2")
    )
    placed = (P("prow", PCOL), P(None, PCOL, "prow"), P(), P())
    return jax.shard_map(
        on_device, mesh=finer, in_specs=placed, out_specs=P("prow", PCOL), check_vma=False
    )
```

```python
import functools

import jax
import jax.numpy as jnp
from jax import lax
from jax.experimental import pallas as pl
from jax.experimental.pallas import tpu as pltpu
from jax.sharding import Mesh
from jax.sharding import PartitionSpec as P

PCOL = ("pcol_0", "pcol_1", "pcol_2")
CHUNK = 1024
PIECE = 1024
F32 = jnp.float32
BF16 = jnp.bfloat16
ROWS_BY_LANES = (((1,), (1,)), ((), ()))
LIMIT = 24 << 20
FETCH_LIMIT = 52 << 20
GRAM_LIMIT = 60 << 20


def exchange(parts, axis):
    return lax.all_to_all(parts, axis, split_axis=0, concat_axis=0, tiled=True)


def copy_for_each(x, axis, devices):
    return exchange(jnp.broadcast_to(x, (devices, *x.shape)), axis)


def from_partner(x):
    return lax.ppermute(x, "pcol_2", [(0, 1), (1, 0)])


def after(x, *earlier):
    return lax.optimization_barrier((x, *earlier))[0]


def two_terms(x):
    high = x.astype(BF16)
    low = (x - high.astype(F32)).astype(BF16)
    return jnp.concatenate([high, low], axis=0)


def folded(x):
    half = x.shape[0] // 2
    return x[:half] + x[half:]


def cost(flops, *operands):
    moved = sum(x.size * x.dtype.itemsize for x in operands)
    return pl.CostEstimate(flops=flops, bytes_accessed=moved, transcendentals=0)


def whole(memory_space=pltpu.VMEM):
    return pl.BlockSpec(memory_space=memory_space)


def local_call(kernel, shapes, flops, *operands, scalars=0):
    single = not isinstance(shapes, (list, tuple))
    return pl.pallas_call(
        kernel,
        out_shape=shapes,
        in_specs=[whole(pltpu.SMEM)] * scalars + [whole()] * (len(operands) - scalars),
        out_specs=whole() if single else [whole()] * len(shapes),
        cost_estimate=cost(flops, *operands),
        compiler_params=pltpu.CompilerParams(vmem_limit_bytes=LIMIT),
    )(*operands)


def fetching_call(kernel, shapes, out_spaces, scratch, flops, far, near):
    return pl.pallas_call(
        kernel,
        out_shape=shapes,
        in_specs=[whole(pltpu.HBM)] * len(far) + [whole()] * len(near),
        out_specs=[whole(space) for space in out_spaces],
        scratch_shapes=scratch,
        cost_estimate=cost(flops, *far, *near),
        compiler_params=pltpu.CompilerParams(vmem_limit_bytes=FETCH_LIMIT),
    )(*far, *near)


def rows_of(ref):
    owners, inner, width = ref.shape
    return ref[...].reshape(owners * inner, width)


def products(reflectors, terms):
    return lax.dot_general(reflectors, terms, ROWS_BY_LANES, preferred_element_type=F32)


def settled(both):
    columns = both.shape[1] // 2
    return (both[:, :columns] + both[:, columns:]).T


def split_kernel(z_ref, turned_ref, terms_ref):
    for i in range(z_ref.shape[0] // CHUNK):
        part = slice(i * CHUNK, (i + 1) * CHUNK)
        turned = z_ref[part, :].T
        turned_ref[:, part] = turned
        terms_ref[:, part] = two_terms(turned)


def first_kernel(terms_ref, half_ref, sums_ref):
    sums_ref[...] = settled(products(half_ref[...], terms_ref[...]))


def second_kernel(terms_ref, half_ref, before_ref, sums_ref):
    size = before_ref.shape[1]
    sums_ref[:, :size] = before_ref[...]
    sums_ref[:, size:] = settled(products(half_ref[...], terms_ref[...]))


def cleared(*refs):
    @pl.when(pl.program_id(0) == 0)
    def _():
        for ref in refs:
            ref[...] = jnp.zeros_like(ref)


def finished(sums_ref, total_ref):
    @pl.when(pl.program_id(0) == pl.num_programs(0) - 1)
    def _():
        sums_ref[...] = settled(total_ref[...])


def early_kernel(
    core_ref, half_ref, high_ref, next_ref, own_ref, partner_ref, terms_ref,
    gram_ref, cross_ref, sums_ref, total_ref,
):
    cleared(gram_ref, cross_ref, total_ref)
    gram_ref[...] += products(rows_of(half_ref), rows_of(high_ref))
    following = rows_of(next_ref)
    used = jnp.concatenate([own_ref[...], partner_ref[...]], axis=0)
    cross_ref[...] += products(following, used)
    total_ref[...] += products(following, terms_ref[...])
    finished(sums_ref, total_ref)


def late_kernel(
    high_ref, low_ref, next_ref, own_ref, partner_ref, terms_ref,
    cross_ref, near_ref, sums_ref, total_ref,
):
    cleared(cross_ref, near_ref, total_ref)
    following = jnp.concatenate([rows_of(high_ref), rows_of(low_ref)], axis=0)
    used = jnp.concatenate([own_ref[...], partner_ref[...]], axis=0)
    cross_ref[...] += products(following, used)
    near_ref[...] += products(following, rows_of(next_ref))
    total_ref[...] += products(following, terms_ref[...])
    finished(sums_ref, total_ref)


def middle_kernel(z_ref, own_ref, partner_ref, next_ref, image_ref, copies_ref, new_ref):
    used = jnp.concatenate([own_ref[...], partner_ref[...], rows_of(next_ref)], axis=0)
    image = jnp.concatenate([image_ref[...], image_of(copies_ref)], axis=1)
    change = jnp.dot(two_terms(image), used, preferred_element_type=F32)
    new_ref[...] = z_ref[...] - folded(change)


def image_of(copies_ref):
    devices, both, size = copies_ref.shape
    return copies_ref[:, : both // 2, :].reshape(devices * both // 2, size)


def stretch(i):
    return slice(i * PIECE, (i + 1) * PIECE)


def fetched(sources, buffers, arrivals):
    copies = []
    for i in range(buffers[0].shape[-1] // PIECE):
        row = []
        for k, (source, buffer) in enumerate(zip(sources, buffers)):
            part = (slice(None),) * (len(buffer.shape) - 1) + (pl.ds(i * PIECE, PIECE),)
            row.append(pltpu.make_async_copy(source.at[part], buffer.at[part], arrivals.at[k, i]))
            row[-1].start()
        copies.append(row)
    return copies


def piece_of(buffer, i):
    if len(buffer.shape) == 2:
        return buffer[:, stretch(i)]
    owners, inner, _ = buffer.shape
    return buffer[:, :, stretch(i)].reshape(owners * inner, PIECE)


def stacked(buffers, i):
    return jnp.concatenate([piece_of(buffer, i) for buffer in buffers], axis=0)


def step_kernel(sums_ref, image_ref, cross_ref, gram_ref, parts_ref):
    devices, both, size = parts_ref.shape
    sums = sums_ref[...] - applied(image_ref[...], cross_ref[...])
    parts_ref[:, : both // 2, :] = sums.reshape(devices, both // 2, size)
    parts_ref[:, both // 2 :, :] = gram_ref[...].reshape(devices, both // 2, size)


def pair_kernel(before_ref, image_ref, cross_ref, copies_ref, near_ref, sums_ref):
    later = applied(image_of(copies_ref), near_ref[...])
    sums_ref[...] = before_ref[...] - applied(image_ref[...], cross_ref[...]) - later


def last_kernel(
    z, gathered, image_ref, result, z_buffer, high_buffer, low_buffer, out_buffer, arrivals, departures
):
    buffers = [z_buffer, high_buffer, low_buffer]
    copies = fetched([z, gathered.at[:, 1], gathered.at[:, 0]], buffers, arrivals)
    terms = two_terms(image_ref[...])

    def leaving(i):
        part = pl.ds(i * PIECE, PIECE)
        return pltpu.make_async_copy(out_buffer.at[part, :], result.at[part, :], departures.at[i])

    for i, row in enumerate(copies):
        for copy in row:
            copy.wait()
        change = jnp.dot(terms, stacked(buffers[1:], i), preferred_element_type=F32)
        out_buffer[stretch(i), :] = (z_buffer[:, stretch(i)] - folded(change)).T
        if i > 0:
            leaving(i - 1).start()
    leaving(len(copies) - 1).start()
    for i in range(len(copies)):
        leaving(i).wait()


def applied(x, matrix):
    return lax.dot_general(
        x, matrix, ROWS_BY_LANES, precision=lax.Precision.HIGHEST, preferred_element_type=F32
    )


def summed(parts_ref):
    total = parts_ref[0]
    for device in range(1, parts_ref.shape[0]):
        total = total + parts_ref[device]
    return total


def share_kernel(parts_ref, tri_ref, copies_ref):
    image = applied(summed(parts_ref), tri_ref[...])
    for device in range(parts_ref.shape[0]):
        copies_ref[device] = image


def gram_share_kernel(parts_ref, tri_ref, copies_ref):
    total = summed(parts_ref)
    rows = total.shape[0] // 2
    image = applied(total[:rows], tri_ref[...])
    for device in range(parts_ref.shape[0]):
        copies_ref[device, :rows] = image
        copies_ref[device, rows:] = total[rows:]


def pair_share_kernel(parts_ref, high_ref, low_ref, gram_ref, copies_ref):
    total = summed(parts_ref)
    size = total.shape[1] // 2
    high = applied(total[:, :size], high_ref[...])
    low = applied(total[:, size:] - applied(high, gram_ref[...]), low_ref[...])
    for device in range(parts_ref.shape[0]):
        copies_ref[device, :, :size] = high
        copies_ref[device, :, size:] = low


def factor_kernel(wide, deep, each, core_ref, tau_ref, coupling_ref, *factor_refs):
    size = tau_ref.shape[1]
    row = lax.broadcasted_iota(jnp.int32, (size, size), 0)
    column = lax.broadcasted_iota(jnp.int32, (size, size), 1)
    spot, inner = row // each, row % each
    high, mid, low = spot // (2 * deep), spot // deep % 2, spot % deep
    together = ((high * deep + low) * 2 + mid) * each + inner
    core = core_ref[0]
    part, rest = row // (size // 2), row % (size // 2)
    parity = jnp.where(part == 0, core, 1 - core)
    across, along = rest // (wide * each), rest % (wide * each) // each
    alone = ((along * deep + across) * 2 + parity) * each + inner
    for position, factor_ref in enumerate(factor_refs):
        wanted = alone if position == len(factor_refs) - 1 else together
        choose = (wanted == column).astype(F32)
        upper = jnp.where(column > row, coupling_ref[position], 0.0)
        factor = jnp.where(column == row, tau_ref[position : position + 1, :], upper)
        turned = jnp.dot(choose, factor, precision=lax.Precision.HIGHEST, preferred_element_type=F32)
        factor_ref[...] = applied(turned, choose)


def on_device(vectors, reflectors, tau_diag, coupling):
    count, each, rows = reflectors.shape
    high_axis, low_axis, core_axis = PCOL
    wide, deep = lax.axis_size(high_axis), lax.axis_size(low_axis)
    devices = lax.axis_size("prow")
    core = lax.axis_index(core_axis)
    last = count - 1
    half = wide * deep * each
    size = 2 * half
    columns = vectors.shape[1]
    share = columns // devices

    def shape(*lengths, dtype=F32):
        return jax.ShapeDtypeStruct(lengths, dtype)

    hopped = copy_for_each(reflectors[:last], low_axis, deep)
    early = hopped.transpose(1, 0, 2, 3).reshape(last, deep * each, rows)
    later = lax.all_gather(early, (high_axis, core_axis), axis=0, tiled=False)

    group = copy_for_each(after(reflectors[last], hopped), high_axis, wide).reshape(wide * each, rows)

    where_core = core.astype(jnp.int32).reshape(1)
    factors = local_call(
        functools.partial(factor_kernel, wide, deep, each),
        [shape(size, size)] * count,
        count * 24 * size**3,
        where_core,
        tau_diag,
        coupling,
        scalars=1,
    )
    current, terms = local_call(
        split_kernel, [shape(columns, rows), shape(2 * columns, rows, dtype=BF16)], 1 << 24, vectors
    )
    start = after(group, current, terms, *factors)
    first = copy_for_each(start, low_axis, deep).reshape(half, rows)
    partner = from_partner(first)

    once = 4 * columns * half * rows
    sums = local_call(first_kernel, shape(columns, half), once, terms, first)
    sums = local_call(second_kernel, shape(columns, size), once, terms, partner, sums)
    arrived = exchange(sums.reshape(devices, share, size), "prow")
    copies = local_call(share_kernel, shape(devices, share, size), 1 << 24, arrived, factors[3])

    gathered = after(later, copies)
    owners, _, inner, _ = gathered.shape
    def panel_at(position, start=None):
        block = (owners if start is None else owners // 2, None, inner, CHUNK)
        if start is None:
            return pl.BlockSpec(block, lambda i, *_: (0, position, 0, i))
        return pl.BlockSpec(block, lambda i, core: (core[0], position, 0, i))

    def by_lanes(lines):
        return pl.BlockSpec((lines, CHUNK), lambda i, *_: (0, i))

    def fixed(*lengths):
        return pl.BlockSpec(lengths, lambda i, *_: (0,) * len(lengths))

    def streamed(kernel, scalars, in_specs, shapes, out_specs, scratch, flops, *operands):
        return pl.pallas_call(
            kernel,
            grid_spec=pltpu.PrefetchScalarGridSpec(
                num_scalar_prefetch=scalars,
                grid=(rows // CHUNK,),
                in_specs=in_specs,
                out_specs=out_specs,
                scratch_shapes=scratch,
            ),
            out_shape=shapes,
            cost_estimate=cost(flops, *operands),
            compiler_params=pltpu.CompilerParams(
                vmem_limit_bytes=GRAM_LIMIT, dimension_semantics=("arbitrary",)
            ),
        )(*operands)

    gram_half, cross, sums = streamed(
        early_kernel,
        1,
        [
            panel_at(0, 0), panel_at(1), panel_at(2),
            by_lanes(half), by_lanes(half), by_lanes(2 * columns),
        ],
        [shape(half, size), shape(size, size), shape(columns, size)],
        [fixed(half, size), fixed(size, size), fixed(columns, size)],
        [pltpu.VMEM((size, 2 * columns), F32)],
        5 * once,
        where_core,
        gathered,
        gathered,
        gathered,
        first,
        partner,
        terms,
    )
    image = exchange(copies, "prow").reshape(columns, size)
    parts = local_call(
        step_kernel, shape(devices, 2 * share, size), 1 << 26, sums, image, cross, gram_half
    )
    arrived = exchange(parts, "prow")
    crosses, nears, sums = streamed(
        late_kernel,
        0,
        [
            panel_at(1), panel_at(0), panel_at(2),
            by_lanes(half), by_lanes(half), by_lanes(2 * columns),
        ],
        [shape(2 * size, size), shape(2 * size, size), shape(columns, 2 * size)],
        [fixed(2 * size, size), fixed(2 * size, size), fixed(columns, 2 * size)],
        [pltpu.VMEM((2 * size, 2 * columns), F32)],
        12 * once,
        gathered,
        gathered,
        gathered,
        first,
        partner,
        terms,
    )
    copies = local_call(gram_share_kernel, shape(*parts.shape), 1 << 24, arrived, factors[2])
    copies = exchange(copies, "prow")
    gram_own = copies[:, share:].reshape(half, size)
    gram_other = from_partner(gram_own)
    gram = jnp.where(
        core == 0,
        jnp.concatenate([gram_own, gram_other]),
        jnp.concatenate([gram_other, gram_own]),
    )
    sums = local_call(
        pair_kernel, shape(columns, 2 * size), 1 << 27, sums, image, crosses, copies, nears
    )
    current = streamed(
        middle_kernel,
        0,
        [
            by_lanes(columns), by_lanes(half), by_lanes(half), panel_at(2),
            fixed(columns, size), fixed(devices, 2 * share, size),
        ],
        shape(columns, rows),
        by_lanes(columns),
        [],
        4 * once,
        current,
        first,
        partner,
        gathered,
        image,
        copies,
    )
    arrived = exchange(sums.reshape(devices, share, 2 * size), "prow")
    copies = local_call(
        pair_share_kernel, shape(*arrived.shape), 1 << 24, arrived, factors[1], factors[0], gram
    )
    image = exchange(copies, "prow").reshape(columns, 2 * size)
    return fetching_call(
        last_kernel,
        [shape(*vectors.shape)],
        [pltpu.HBM],
        [
            pltpu.VMEM((columns, rows), F32),
            pltpu.VMEM((owners, inner, rows), BF16),
            pltpu.VMEM((owners, inner, rows), BF16),
            pltpu.VMEM(vectors.shape, F32),
            pltpu.SemaphoreType.DMA((3, rows // PIECE)),
            pltpu.SemaphoreType.DMA((rows // PIECE,)),
        ],
        4 * once,
        [current, gathered],
        [image],
    )[0]


def solution(mesh):
    finer = Mesh(
        mesh.devices.reshape(mesh.shape["prow"], 8, 4, 2), ("prow", "pcol_0", "pcol_1", "pcol_2")
    )
    placed = (P("prow", PCOL), P(None, PCOL, "prow"), P(), P())
    return jax.shard_map(
        on_device, mesh=finer, in_specs=placed, out_specs=P("prow", PCOL), check_vma=False
    )
```

```python
import functools

import jax
import jax.numpy as jnp
from jax import lax
from jax.experimental import pallas as pl
from jax.experimental.pallas import tpu as pltpu
from jax.sharding import Mesh
from jax.sharding import PartitionSpec as P

PCOL = ("pcol_0", "pcol_1", "pcol_2")
CHUNK = 1024
PIECE = 1024
F32 = jnp.float32
BF16 = jnp.bfloat16
ROWS_BY_LANES = (((1,), (1,)), ((), ()))
LIMIT = 24 << 20
FETCH_LIMIT = 52 << 20
GRAM_LIMIT = 52 << 20


def exchange(parts, axis):
    return lax.all_to_all(parts, axis, split_axis=0, concat_axis=0, tiled=True)


def copy_for_each(x, axis, devices):
    return exchange(jnp.broadcast_to(x, (devices, *x.shape)), axis)


def from_partner(x):
    return lax.ppermute(x, "pcol_2", [(0, 1), (1, 0)])


def after(x, *earlier):
    return lax.optimization_barrier((x, *earlier))[0]


def two_terms(x):
    high = x.astype(BF16)
    low = (x - high.astype(F32)).astype(BF16)
    return jnp.concatenate([high, low], axis=0)


def folded(x):
    half = x.shape[0] // 2
    return x[:half] + x[half:]


def cost(flops, *operands):
    moved = sum(x.size * x.dtype.itemsize for x in operands)
    return pl.CostEstimate(flops=flops, bytes_accessed=moved, transcendentals=0)


def whole(memory_space=pltpu.VMEM):
    return pl.BlockSpec(memory_space=memory_space)


def local_call(kernel, shapes, flops, *operands, scalars=0):
    single = not isinstance(shapes, (list, tuple))
    return pl.pallas_call(
        kernel,
        out_shape=shapes,
        in_specs=[whole(pltpu.SMEM)] * scalars + [whole()] * (len(operands) - scalars),
        out_specs=whole() if single else [whole()] * len(shapes),
        cost_estimate=cost(flops, *operands),
        compiler_params=pltpu.CompilerParams(vmem_limit_bytes=LIMIT),
    )(*operands)


def fetching_call(kernel, shapes, out_spaces, scratch, flops, far, near):
    return pl.pallas_call(
        kernel,
        out_shape=shapes,
        in_specs=[whole(pltpu.HBM)] * len(far) + [whole()] * len(near),
        out_specs=[whole(space) for space in out_spaces],
        scratch_shapes=scratch,
        cost_estimate=cost(flops, *far, *near),
        compiler_params=pltpu.CompilerParams(vmem_limit_bytes=FETCH_LIMIT),
    )(*far, *near)


def rows_of(ref):
    owners, inner, width = ref.shape
    return ref[...].reshape(owners * inner, width)


def products(reflectors, terms):
    return lax.dot_general(reflectors, terms, ROWS_BY_LANES, preferred_element_type=F32)


def settled(both):
    columns = both.shape[1] // 2
    return (both[:, :columns] + both[:, columns:]).T


def split_kernel(z_ref, turned_ref, terms_ref):
    for i in range(z_ref.shape[0] // CHUNK):
        part = slice(i * CHUNK, (i + 1) * CHUNK)
        turned = z_ref[part, :].T
        turned_ref[:, part] = turned
        terms_ref[:, part] = two_terms(turned)


def first_kernel(terms_ref, half_ref, sums_ref):
    sums_ref[...] = settled(products(half_ref[...], terms_ref[...]))


def second_kernel(terms_ref, half_ref, before_ref, sums_ref):
    size = before_ref.shape[1]
    sums_ref[:, :size] = before_ref[...]
    sums_ref[:, size:] = settled(products(half_ref[...], terms_ref[...]))


def cleared(*refs):
    @pl.when(pl.program_id(0) == 0)
    def _():
        for ref in refs:
            ref[...] = jnp.zeros_like(ref)


def finished(sums_ref, total_ref):
    @pl.when(pl.program_id(0) == pl.num_programs(0) - 1)
    def _():
        sums_ref[...] = settled(total_ref[...])


def early_kernel(
    core_ref, half_ref, high_ref, next_ref, own_ref, partner_ref, terms_ref,
    gram_ref, cross_ref, sums_ref, total_ref,
):
    cleared(gram_ref, cross_ref, total_ref)
    gram_ref[...] += products(rows_of(half_ref), rows_of(high_ref))
    following = rows_of(next_ref)
    used = jnp.concatenate([own_ref[...], partner_ref[...]], axis=0)
    cross_ref[...] += products(following, used)
    total_ref[...] += products(following, terms_ref[...])
    finished(sums_ref, total_ref)


def late_kernel(
    high_ref, low_ref, next_ref, own_ref, partner_ref, terms_ref,
    cross_ref, near_ref, sums_ref, total_ref,
):
    cleared(cross_ref, near_ref, total_ref)
    following = jnp.concatenate([rows_of(high_ref), rows_of(low_ref)], axis=0)
    used = jnp.concatenate([own_ref[...], partner_ref[...]], axis=0)
    cross_ref[...] += products(following, used)
    near_ref[...] += products(following, rows_of(next_ref))
    total_ref[...] += products(following, terms_ref[...])
    finished(sums_ref, total_ref)


def middle_kernel(z_ref, own_ref, partner_ref, next_ref, image_ref, copies_ref, new_ref):
    used = jnp.concatenate([own_ref[...], partner_ref[...], rows_of(next_ref)], axis=0)
    image = jnp.concatenate([image_ref[...], image_of(copies_ref)], axis=1)
    change = jnp.dot(two_terms(image), used, preferred_element_type=F32)
    new_ref[...] = z_ref[...] - folded(change)


def image_of(copies_ref):
    devices, both, size = copies_ref.shape
    return copies_ref[:, : both // 2, :].reshape(devices * both // 2, size)


def stretch(i):
    return slice(i * PIECE, (i + 1) * PIECE)


def fetched(sources, buffers, arrivals):
    copies = []
    for i in range(buffers[0].shape[-1] // PIECE):
        row = []
        for k, (source, buffer) in enumerate(zip(sources, buffers)):
            part = (slice(None),) * (len(buffer.shape) - 1) + (pl.ds(i * PIECE, PIECE),)
            row.append(pltpu.make_async_copy(source.at[part], buffer.at[part], arrivals.at[k, i]))
            row[-1].start()
        copies.append(row)
    return copies


def piece_of(buffer, i):
    if len(buffer.shape) == 2:
        return buffer[:, stretch(i)]
    owners, inner, _ = buffer.shape
    return buffer[:, :, stretch(i)].reshape(owners * inner, PIECE)


def stacked(buffers, i):
    return jnp.concatenate([piece_of(buffer, i) for buffer in buffers], axis=0)


def step_kernel(sums_ref, image_ref, cross_ref, gram_ref, parts_ref):
    devices, both, size = parts_ref.shape
    sums = sums_ref[...] - applied(image_ref[...], cross_ref[...])
    parts_ref[:, : both // 2, :] = sums.reshape(devices, both // 2, size)
    parts_ref[:, both // 2 :, :] = gram_ref[...].reshape(devices, both // 2, size)


def pair_kernel(before_ref, image_ref, cross_ref, copies_ref, near_ref, sums_ref):
    later = applied(image_of(copies_ref), near_ref[...])
    sums_ref[...] = before_ref[...] - applied(image_ref[...], cross_ref[...]) - later


def last_kernel(
    z, gathered, image_ref, result, z_buffer, high_buffer, low_buffer, out_buffer, arrivals, departures
):
    buffers = [z_buffer, high_buffer, low_buffer]
    copies = fetched([z, gathered.at[:, 1], gathered.at[:, 0]], buffers, arrivals)
    terms = two_terms(image_ref[...])

    def leaving(i):
        part = pl.ds(i * PIECE, PIECE)
        return pltpu.make_async_copy(out_buffer.at[part, :], result.at[part, :], departures.at[i])

    for i, row in enumerate(copies):
        for copy in row:
            copy.wait()
        change = jnp.dot(terms, stacked(buffers[1:], i), preferred_element_type=F32)
        out_buffer[stretch(i), :] = (z_buffer[:, stretch(i)] - folded(change)).T
        if i > 0:
            leaving(i - 1).start()
    leaving(len(copies) - 1).start()
    for i in range(len(copies)):
        leaving(i).wait()


def applied(x, matrix):
    return lax.dot_general(
        x, matrix, ROWS_BY_LANES, precision=lax.Precision.HIGHEST, preferred_element_type=F32
    )


def summed(parts_ref):
    total = parts_ref[0]
    for device in range(1, parts_ref.shape[0]):
        total = total + parts_ref[device]
    return total


def share_kernel(parts_ref, tri_ref, copies_ref):
    image = applied(summed(parts_ref), tri_ref[...])
    for device in range(parts_ref.shape[0]):
        copies_ref[device] = image


def gram_share_kernel(parts_ref, tri_ref, copies_ref):
    total = summed(parts_ref)
    rows = total.shape[0] // 2
    image = applied(total[:rows], tri_ref[...])
    for device in range(parts_ref.shape[0]):
        copies_ref[device, :rows] = image
        copies_ref[device, rows:] = total[rows:]


def pair_share_kernel(parts_ref, high_ref, low_ref, gram_ref, copies_ref):
    total = summed(parts_ref)
    size = total.shape[1] // 2
    high = applied(total[:, :size], high_ref[...])
    low = applied(total[:, size:] - applied(high, gram_ref[...]), low_ref[...])
    for device in range(parts_ref.shape[0]):
        copies_ref[device, :, :size] = high
        copies_ref[device, :, size:] = low


def factor_kernel(wide, deep, each, core_ref, tau_ref, coupling_ref, *factor_refs):
    size = tau_ref.shape[1]
    row = lax.broadcasted_iota(jnp.int32, (size, size), 0)
    column = lax.broadcasted_iota(jnp.int32, (size, size), 1)
    spot, inner = row // each, row % each
    high, mid, low = spot // (2 * deep), spot // deep % 2, spot % deep
    together = ((high * deep + low) * 2 + mid) * each + inner
    core = core_ref[0]
    part, rest = row // (size // 2), row % (size // 2)
    parity = jnp.where(part == 0, core, 1 - core)
    across, along = rest // (wide * each), rest % (wide * each) // each
    alone = ((along * deep + across) * 2 + parity) * each + inner
    for position, factor_ref in enumerate(factor_refs):
        wanted = alone if position == len(factor_refs) - 1 else together
        choose = (wanted == column).astype(F32)
        upper = jnp.where(column > row, coupling_ref[position], 0.0)
        factor = jnp.where(column == row, tau_ref[position : position + 1, :], upper)
        turned = jnp.dot(choose, factor, precision=lax.Precision.HIGHEST, preferred_element_type=F32)
        factor_ref[...] = applied(turned, choose)


def on_device(vectors, reflectors, tau_diag, coupling):
    count, each, rows = reflectors.shape
    high_axis, low_axis, core_axis = PCOL
    wide, deep = lax.axis_size(high_axis), lax.axis_size(low_axis)
    devices = lax.axis_size("prow")
    core = lax.axis_index(core_axis)
    last = count - 1
    half = wide * deep * each
    size = 2 * half
    columns = vectors.shape[1]
    share = columns // devices

    def shape(*lengths, dtype=F32):
        return jax.ShapeDtypeStruct(lengths, dtype)

    hopped = copy_for_each(reflectors[:last], low_axis, deep)
    early = hopped.transpose(1, 0, 2, 3).reshape(last, deep * each, rows)
    later = lax.all_gather(early, (high_axis, core_axis), axis=0, tiled=False)

    group = copy_for_each(after(reflectors[last], hopped), high_axis, wide).reshape(wide * each, rows)

    where_core = core.astype(jnp.int32).reshape(1)
    factors = local_call(
        functools.partial(factor_kernel, wide, deep, each),
        [shape(size, size)] * count,
        count * 24 * size**3,
        where_core,
        tau_diag,
        coupling,
        scalars=1,
    )
    current, terms = local_call(
        split_kernel, [shape(columns, rows), shape(2 * columns, rows, dtype=BF16)], 1 << 24, vectors
    )
    start = after(group, current, terms, *factors)
    first = copy_for_each(start, low_axis, deep).reshape(half, rows)
    partner = from_partner(first)

    once = 4 * columns * half * rows
    sums = local_call(first_kernel, shape(columns, half), once, terms, first)
    sums = local_call(second_kernel, shape(columns, size), once, terms, partner, sums)
    arrived = exchange(sums.reshape(devices, share, size), "prow")
    copies = local_call(share_kernel, shape(devices, share, size), 1 << 24, arrived, factors[3])

    gathered = after(later, copies)
    owners, _, inner, _ = gathered.shape
    def panel_at(position, start=None):
        block = (owners if start is None else owners // 2, None, inner, CHUNK)
        if start is None:
            return pl.BlockSpec(block, lambda i, *_: (0, position, 0, i))
        return pl.BlockSpec(block, lambda i, core: (core[0], position, 0, i))

    def by_lanes(lines):
        return pl.BlockSpec((lines, CHUNK), lambda i, *_: (0, i))

    def fixed(*lengths):
        return pl.BlockSpec(lengths, lambda i, *_: (0,) * len(lengths))

    def streamed(kernel, scalars, in_specs, shapes, out_specs, scratch, flops, *operands):
        return pl.pallas_call(
            kernel,
            grid_spec=pltpu.PrefetchScalarGridSpec(
                num_scalar_prefetch=scalars,
                grid=(rows // CHUNK,),
                in_specs=in_specs,
                out_specs=out_specs,
                scratch_shapes=scratch,
            ),
            out_shape=shapes,
            cost_estimate=cost(flops, *operands),
            compiler_params=pltpu.CompilerParams(
                vmem_limit_bytes=GRAM_LIMIT, dimension_semantics=("arbitrary",)
            ),
        )(*operands)

    gram_half, cross, sums = streamed(
        early_kernel,
        1,
        [
            panel_at(0, 0), panel_at(1), panel_at(2),
            by_lanes(half), by_lanes(half), by_lanes(2 * columns),
        ],
        [shape(half, size), shape(size, size), shape(columns, size)],
        [fixed(half, size), fixed(size, size), fixed(columns, size)],
        [pltpu.VMEM((size, 2 * columns), F32)],
        5 * once,
        where_core,
        gathered,
        gathered,
        gathered,
        first,
        partner,
        terms,
    )
    image = exchange(copies, "prow").reshape(columns, size)
    parts = local_call(
        step_kernel, shape(devices, 2 * share, size), 1 << 26, sums, image, cross, gram_half
    )
    arrived = exchange(parts, "prow")
    crosses, nears, sums = streamed(
        late_kernel,
        0,
        [
            panel_at(1), panel_at(0), panel_at(2),
            by_lanes(half), by_lanes(half), by_lanes(2 * columns),
        ],
        [shape(2 * size, size), shape(2 * size, size), shape(columns, 2 * size)],
        [fixed(2 * size, size), fixed(2 * size, size), fixed(columns, 2 * size)],
        [pltpu.VMEM((2 * size, 2 * columns), F32)],
        12 * once,
        gathered,
        gathered,
        gathered,
        first,
        partner,
        terms,
    )
    copies = local_call(gram_share_kernel, shape(*parts.shape), 1 << 24, arrived, factors[2])
    copies = exchange(copies, "prow")
    gram_own = copies[:, share:].reshape(half, size)
    gram_other = from_partner(gram_own)
    gram = jnp.where(
        core == 0,
        jnp.concatenate([gram_own, gram_other]),
        jnp.concatenate([gram_other, gram_own]),
    )
    sums = local_call(
        pair_kernel, shape(columns, 2 * size), 1 << 27, sums, image, crosses, copies, nears
    )
    current = streamed(
        middle_kernel,
        0,
        [
            by_lanes(columns), by_lanes(half), by_lanes(half), panel_at(2),
            fixed(columns, size), fixed(devices, 2 * share, size),
        ],
        shape(columns, rows),
        by_lanes(columns),
        [],
        4 * once,
        current,
        first,
        partner,
        gathered,
        image,
        copies,
    )
    arrived = exchange(sums.reshape(devices, share, 2 * size), "prow")
    copies = local_call(
        pair_share_kernel, shape(*arrived.shape), 1 << 24, arrived, factors[1], factors[0], gram
    )
    image = exchange(copies, "prow").reshape(columns, 2 * size)
    return fetching_call(
        last_kernel,
        [shape(*vectors.shape)],
        [pltpu.HBM],
        [
            pltpu.VMEM((columns, rows), F32),
            pltpu.VMEM((owners, inner, rows), BF16),
            pltpu.VMEM((owners, inner, rows), BF16),
            pltpu.VMEM(vectors.shape, F32),
            pltpu.SemaphoreType.DMA((3, rows // PIECE)),
            pltpu.SemaphoreType.DMA((rows // PIECE,)),
        ],
        4 * once,
        [current, gathered],
        [image],
    )[0]


def solution(mesh):
    finer = Mesh(
        mesh.devices.reshape(mesh.shape["prow"], 8, 4, 2), ("prow", "pcol_0", "pcol_1", "pcol_2")
    )
    placed = (P("prow", PCOL), P(None, PCOL, "prow"), P(), P())
    return jax.shard_map(
        on_device, mesh=finer, in_specs=placed, out_specs=P("prow", PCOL), check_vma=False
    )
```

```python
import functools

import jax
import jax.numpy as jnp
from jax import lax
from jax.experimental import pallas as pl
from jax.experimental.pallas import tpu as pltpu
from jax.sharding import Mesh
from jax.sharding import PartitionSpec as P

PCOL = ("pcol_0", "pcol_1", "pcol_2")
CHUNK = 1024
PIECE = 1024
F32 = jnp.float32
BF16 = jnp.bfloat16
ROWS_BY_LANES = (((1,), (1,)), ((), ()))
LIMIT = 24 << 20
FETCH_LIMIT = 52 << 20
GRAM_LIMIT = 52 << 20


def exchange(parts, axis):
    return lax.all_to_all(parts, axis, split_axis=0, concat_axis=0, tiled=True)


def copy_for_each(x, axis, devices):
    return exchange(jnp.broadcast_to(x, (devices, *x.shape)), axis)


def from_partner(x):
    return lax.ppermute(x, "pcol_2", [(0, 1), (1, 0)])


def after(x, *earlier):
    return lax.optimization_barrier((x, *earlier))[0]


def two_terms(x):
    high = x.astype(BF16)
    low = (x - high.astype(F32)).astype(BF16)
    return jnp.concatenate([high, low], axis=0)


def folded(x):
    half = x.shape[0] // 2
    return x[:half] + x[half:]


def cost(flops, *operands):
    moved = sum(x.size * x.dtype.itemsize for x in operands)
    return pl.CostEstimate(flops=flops, bytes_accessed=moved, transcendentals=0)


def whole(memory_space=pltpu.VMEM):
    return pl.BlockSpec(memory_space=memory_space)


def local_call(kernel, shapes, flops, *operands, scalars=0):
    single = not isinstance(shapes, (list, tuple))
    return pl.pallas_call(
        kernel,
        out_shape=shapes,
        in_specs=[whole(pltpu.SMEM)] * scalars + [whole()] * (len(operands) - scalars),
        out_specs=whole() if single else [whole()] * len(shapes),
        cost_estimate=cost(flops, *operands),
        compiler_params=pltpu.CompilerParams(vmem_limit_bytes=LIMIT),
    )(*operands)


def fetching_call(kernel, shapes, out_spaces, scratch, flops, far, near):
    return pl.pallas_call(
        kernel,
        out_shape=shapes,
        in_specs=[whole(pltpu.HBM)] * len(far) + [whole()] * len(near),
        out_specs=[whole(space) for space in out_spaces],
        scratch_shapes=scratch,
        cost_estimate=cost(flops, *far, *near),
        compiler_params=pltpu.CompilerParams(vmem_limit_bytes=FETCH_LIMIT),
    )(*far, *near)


def rows_of(ref):
    owners, inner, width = ref.shape
    return ref[...].reshape(owners * inner, width)


def products(reflectors, terms):
    return lax.dot_general(reflectors, terms, ROWS_BY_LANES, preferred_element_type=F32)


def settled(both):
    columns = both.shape[1] // 2
    return (both[:, :columns] + both[:, columns:]).T


def split_kernel(z_ref, turned_ref, terms_ref):
    for i in range(z_ref.shape[0] // CHUNK):
        part = slice(i * CHUNK, (i + 1) * CHUNK)
        turned = z_ref[part, :].T
        turned_ref[:, part] = turned
        terms_ref[:, part] = two_terms(turned)


def first_kernel(terms_ref, half_ref, sums_ref):
    sums_ref[...] = settled(products(half_ref[...], terms_ref[...]))


def second_kernel(terms_ref, half_ref, before_ref, sums_ref):
    size = before_ref.shape[1]
    sums_ref[:, :size] = before_ref[...]
    sums_ref[:, size:] = settled(products(half_ref[...], terms_ref[...]))


def cleared(*refs):
    @pl.when(pl.program_id(0) == 0)
    def _():
        for ref in refs:
            ref[...] = jnp.zeros_like(ref)


def finished(sums_ref, total_ref):
    @pl.when(pl.program_id(0) == pl.num_programs(0) - 1)
    def _():
        sums_ref[...] = settled(total_ref[...])


def early_kernel(
    core_ref, half_ref, high_ref, next_ref, own_ref, partner_ref, terms_ref,
    gram_ref, cross_ref, sums_ref, total_ref,
):
    cleared(gram_ref, cross_ref, total_ref)
    gram_ref[...] += products(rows_of(half_ref), rows_of(high_ref))
    following = rows_of(next_ref)
    used = jnp.concatenate([own_ref[...], partner_ref[...]], axis=0)
    cross_ref[...] += products(following, used)
    total_ref[...] += products(following, terms_ref[...])
    finished(sums_ref, total_ref)


def late_kernel(
    high_ref, low_ref, next_ref, own_ref, partner_ref, terms_ref, image_ref,
    near_ref, sums_ref, cross_ref, total_ref,
):
    cleared(cross_ref, near_ref, total_ref)
    following = jnp.concatenate([rows_of(high_ref), rows_of(low_ref)], axis=0)
    used = jnp.concatenate([own_ref[...], partner_ref[...]], axis=0)
    cross_ref[...] += products(following, used)
    near_ref[...] += products(following, rows_of(next_ref))
    total_ref[...] += products(following, terms_ref[...])

    @pl.when(pl.program_id(0) == pl.num_programs(0) - 1)
    def _():
        sums_ref[...] = settled(total_ref[...]) - applied(image_ref[...], cross_ref[...])


def middle_kernel(z_ref, own_ref, partner_ref, next_ref, image_ref, copies_ref, new_ref):
    used = jnp.concatenate([own_ref[...], partner_ref[...], rows_of(next_ref)], axis=0)
    image = jnp.concatenate([image_ref[...], image_of(copies_ref)], axis=1)
    change = jnp.dot(two_terms(image), used, preferred_element_type=F32)
    new_ref[...] = z_ref[...] - folded(change)


def image_of(copies_ref):
    devices, both, size = copies_ref.shape
    return copies_ref[:, : both // 2, :].reshape(devices * both // 2, size)


def stretch(i):
    return slice(i * PIECE, (i + 1) * PIECE)


def fetched(sources, buffers, arrivals):
    copies = []
    for i in range(buffers[0].shape[-1] // PIECE):
        row = []
        for k, (source, buffer) in enumerate(zip(sources, buffers)):
            part = (slice(None),) * (len(buffer.shape) - 1) + (pl.ds(i * PIECE, PIECE),)
            row.append(pltpu.make_async_copy(source.at[part], buffer.at[part], arrivals.at[k, i]))
            row[-1].start()
        copies.append(row)
    return copies


def piece_of(buffer, i):
    if len(buffer.shape) == 2:
        return buffer[:, stretch(i)]
    owners, inner, _ = buffer.shape
    return buffer[:, :, stretch(i)].reshape(owners * inner, PIECE)


def stacked(buffers, i):
    return jnp.concatenate([piece_of(buffer, i) for buffer in buffers], axis=0)


def step_kernel(sums_ref, image_ref, cross_ref, gram_ref, parts_ref):
    devices, both, size = parts_ref.shape
    sums = sums_ref[...] - applied(image_ref[...], cross_ref[...])
    parts_ref[:, : both // 2, :] = sums.reshape(devices, both // 2, size)
    parts_ref[:, both // 2 :, :] = gram_ref[...].reshape(devices, both // 2, size)


def pair_kernel(before_ref, copies_ref, near_ref, sums_ref):
    sums_ref[...] = before_ref[...] - applied(image_of(copies_ref), near_ref[...])


def last_kernel(
    z, gathered, image_ref, result, z_buffer, high_buffer, low_buffer, out_buffer, arrivals, departures
):
    buffers = [z_buffer, high_buffer, low_buffer]
    copies = fetched([z, gathered.at[:, 1], gathered.at[:, 0]], buffers, arrivals)
    terms = two_terms(image_ref[...])

    def leaving(i):
        part = pl.ds(i * PIECE, PIECE)
        return pltpu.make_async_copy(out_buffer.at[part, :], result.at[part, :], departures.at[i])

    for i, row in enumerate(copies):
        for copy in row:
            copy.wait()
        change = jnp.dot(terms, stacked(buffers[1:], i), preferred_element_type=F32)
        out_buffer[stretch(i), :] = (z_buffer[:, stretch(i)] - folded(change)).T
        if i > 0:
            leaving(i - 1).start()
    leaving(len(copies) - 1).start()
    for i in range(len(copies)):
        leaving(i).wait()


def applied(x, matrix):
    return lax.dot_general(
        x, matrix, ROWS_BY_LANES, precision=lax.Precision.HIGHEST, preferred_element_type=F32
    )


def summed(parts_ref):
    total = parts_ref[0]
    for device in range(1, parts_ref.shape[0]):
        total = total + parts_ref[device]
    return total


def share_kernel(parts_ref, tri_ref, copies_ref):
    image = applied(summed(parts_ref), tri_ref[...])
    for device in range(parts_ref.shape[0]):
        copies_ref[device] = image


def gram_share_kernel(parts_ref, tri_ref, copies_ref):
    total = summed(parts_ref)
    rows = total.shape[0] // 2
    image = applied(total[:rows], tri_ref[...])
    for device in range(parts_ref.shape[0]):
        copies_ref[device, :rows] = image
        copies_ref[device, rows:] = total[rows:]


def pair_share_kernel(parts_ref, high_ref, low_ref, gram_ref, copies_ref):
    total = summed(parts_ref)
    size = total.shape[1] // 2
    high = applied(total[:, :size], high_ref[...])
    low = applied(total[:, size:] - applied(high, gram_ref[...]), low_ref[...])
    for device in range(parts_ref.shape[0]):
        copies_ref[device, :, :size] = high
        copies_ref[device, :, size:] = low


def factor_kernel(wide, deep, each, core_ref, tau_ref, coupling_ref, *factor_refs):
    size = tau_ref.shape[1]
    row = lax.broadcasted_iota(jnp.int32, (size, size), 0)
    column = lax.broadcasted_iota(jnp.int32, (size, size), 1)
    spot, inner = row // each, row % each
    high, mid, low = spot // (2 * deep), spot // deep % 2, spot % deep
    together = ((high * deep + low) * 2 + mid) * each + inner
    core = core_ref[0]
    part, rest = row // (size // 2), row % (size // 2)
    parity = jnp.where(part == 0, core, 1 - core)
    across, along = rest // (wide * each), rest % (wide * each) // each
    alone = ((along * deep + across) * 2 + parity) * each + inner
    for position, factor_ref in enumerate(factor_refs):
        wanted = alone if position == len(factor_refs) - 1 else together
        choose = (wanted == column).astype(F32)
        upper = jnp.where(column > row, coupling_ref[position], 0.0)
        factor = jnp.where(column == row, tau_ref[position : position + 1, :], upper)
        turned = jnp.dot(choose, factor, precision=lax.Precision.HIGHEST, preferred_element_type=F32)
        factor_ref[...] = applied(turned, choose)


def on_device(vectors, reflectors, tau_diag, coupling):
    count, each, rows = reflectors.shape
    high_axis, low_axis, core_axis = PCOL
    wide, deep = lax.axis_size(high_axis), lax.axis_size(low_axis)
    devices = lax.axis_size("prow")
    core = lax.axis_index(core_axis)
    last = count - 1
    half = wide * deep * each
    size = 2 * half
    columns = vectors.shape[1]
    share = columns // devices

    def shape(*lengths, dtype=F32):
        return jax.ShapeDtypeStruct(lengths, dtype)

    hopped = copy_for_each(reflectors[:last], low_axis, deep)
    early = hopped.transpose(1, 0, 2, 3).reshape(last, deep * each, rows)
    later = lax.all_gather(early, (high_axis, core_axis), axis=0, tiled=False)

    group = copy_for_each(after(reflectors[last], hopped), high_axis, wide).reshape(wide * each, rows)

    where_core = core.astype(jnp.int32).reshape(1)
    factors = local_call(
        functools.partial(factor_kernel, wide, deep, each),
        [shape(size, size)] * count,
        count * 24 * size**3,
        where_core,
        tau_diag,
        coupling,
        scalars=1,
    )
    current, terms = local_call(
        split_kernel, [shape(columns, rows), shape(2 * columns, rows, dtype=BF16)], 1 << 24, vectors
    )
    start = after(group, current, terms, *factors)
    first = copy_for_each(start, low_axis, deep).reshape(half, rows)
    partner = from_partner(first)

    once = 4 * columns * half * rows
    sums = local_call(first_kernel, shape(columns, half), once, terms, first)
    sums = local_call(second_kernel, shape(columns, size), once, terms, partner, sums)
    arrived = exchange(sums.reshape(devices, share, size), "prow")
    copies = local_call(share_kernel, shape(devices, share, size), 1 << 24, arrived, factors[3])

    gathered = after(later, copies)
    owners, _, inner, _ = gathered.shape
    def panel_at(position, start=None):
        block = (owners if start is None else owners // 2, None, inner, CHUNK)
        if start is None:
            return pl.BlockSpec(block, lambda i, *_: (0, position, 0, i))
        return pl.BlockSpec(block, lambda i, core: (core[0], position, 0, i))

    def by_lanes(lines):
        return pl.BlockSpec((lines, CHUNK), lambda i, *_: (0, i))

    def fixed(*lengths):
        return pl.BlockSpec(lengths, lambda i, *_: (0,) * len(lengths))

    def streamed(kernel, scalars, in_specs, shapes, out_specs, scratch, flops, *operands):
        return pl.pallas_call(
            kernel,
            grid_spec=pltpu.PrefetchScalarGridSpec(
                num_scalar_prefetch=scalars,
                grid=(rows // CHUNK,),
                in_specs=in_specs,
                out_specs=out_specs,
                scratch_shapes=scratch,
            ),
            out_shape=shapes,
            cost_estimate=cost(flops, *operands),
            compiler_params=pltpu.CompilerParams(
                vmem_limit_bytes=GRAM_LIMIT, dimension_semantics=("arbitrary",)
            ),
        )(*operands)

    gram_half, cross, sums = streamed(
        early_kernel,
        1,
        [
            panel_at(0, 0), panel_at(1), panel_at(2),
            by_lanes(half), by_lanes(half), by_lanes(2 * columns),
        ],
        [shape(half, size), shape(size, size), shape(columns, size)],
        [fixed(half, size), fixed(size, size), fixed(columns, size)],
        [pltpu.VMEM((size, 2 * columns), F32)],
        5 * once,
        where_core,
        gathered,
        gathered,
        gathered,
        first,
        partner,
        terms,
    )
    image = exchange(copies, "prow").reshape(columns, size)
    parts = local_call(
        step_kernel, shape(devices, 2 * share, size), 1 << 26, sums, image, cross, gram_half
    )
    arrived = exchange(parts, "prow")
    nears, sums = streamed(
        late_kernel,
        0,
        [
            panel_at(1), panel_at(0), panel_at(2),
            by_lanes(half), by_lanes(half), by_lanes(2 * columns),
            fixed(columns, size),
        ],
        [shape(2 * size, size), shape(columns, 2 * size)],
        [fixed(2 * size, size), fixed(columns, 2 * size)],
        [pltpu.VMEM((2 * size, size), F32), pltpu.VMEM((2 * size, 2 * columns), F32)],
        12 * once,
        gathered,
        gathered,
        gathered,
        first,
        partner,
        terms,
        image,
    )
    copies = local_call(gram_share_kernel, shape(*parts.shape), 1 << 24, arrived, factors[2])
    copies = exchange(copies, "prow")
    gram_own = copies[:, share:].reshape(half, size)
    gram_other = from_partner(gram_own)
    gram = jnp.where(
        core == 0,
        jnp.concatenate([gram_own, gram_other]),
        jnp.concatenate([gram_other, gram_own]),
    )
    sums = local_call(
        pair_kernel, shape(columns, 2 * size), 1 << 27, sums, copies, nears
    )
    current = streamed(
        middle_kernel,
        0,
        [
            by_lanes(columns), by_lanes(half), by_lanes(half), panel_at(2),
            fixed(columns, size), fixed(devices, 2 * share, size),
        ],
        shape(columns, rows),
        by_lanes(columns),
        [],
        4 * once,
        current,
        first,
        partner,
        gathered,
        image,
        copies,
    )
    arrived = exchange(sums.reshape(devices, share, 2 * size), "prow")
    copies = local_call(
        pair_share_kernel, shape(*arrived.shape), 1 << 24, arrived, factors[1], factors[0], gram
    )
    image = exchange(copies, "prow").reshape(columns, 2 * size)
    return fetching_call(
        last_kernel,
        [shape(*vectors.shape)],
        [pltpu.HBM],
        [
            pltpu.VMEM((columns, rows), F32),
            pltpu.VMEM((owners, inner, rows), BF16),
            pltpu.VMEM((owners, inner, rows), BF16),
            pltpu.VMEM(vectors.shape, F32),
            pltpu.SemaphoreType.DMA((3, rows // PIECE)),
            pltpu.SemaphoreType.DMA((rows // PIECE,)),
        ],
        4 * once,
        [current, gathered],
        [image],
    )[0]


def solution(mesh):
    finer = Mesh(
        mesh.devices.reshape(mesh.shape["prow"], 8, 4, 2), ("prow", "pcol_0", "pcol_1", "pcol_2")
    )
    placed = (P("prow", PCOL), P(None, PCOL, "prow"), P(), P())
    return jax.shard_map(
        on_device, mesh=finer, in_specs=placed, out_specs=P("prow", PCOL), check_vma=False
    )
```
